256 devices in a mesh: tm: 64 (over y, z, core), space: 4 (over x).
Axes of the slice: x: 4, y: 4, z: 8, core: 2. Of those that a mesh axis runs over, the one named last changes fastest.
Arguments:
- residual: float32 [64, 2, 1024, 1024], P('tm', None, 'space'), may hold values from -0.875 to 0.875
- counts: int32 [64], P('tm'), may hold values from 1 to 4
Outputs:
- fields: float32 [64, 2, 1024, 1024], P('tm', None, 'space')
The draws below stay inside these ranges and needn't reach their ends.
All inputs are finite; a program needn't handle non-finite values.
Results may differ from the reference program's by a relative error of at most 0.0003.
Values sent between devices are 32-bit elements; how exact they have to be, the bound alone decides.
A program may use at most 320 MiB of HBM per device.

```python
import jax
import jax.numpy as jnp
from jax import lax

NX = 1024
NY = 1024
NT = 64


def set_ends(array, stream_key, least, high):
    longest = array.shape.index(max(array.shape))
    spots = []
    for shift in (0, 1):
        where = [jax.random.randint(jax.random.fold_in(stream_key, axis), (), 0, length) for axis, length in enumerate(array.shape)]
        where[longest] = (where[longest] + shift) % array.shape[longest]
        spots.append(tuple(where))
    return array.at[spots[0]].set(least).at[spots[1]].set(high)


def block_scale(rng, shape, shards, low, high):
    level, own = 1.0, jax.random.fold_in(rng, 6)
    for position, shards_of in shards:
        draws = jnp.exp(jax.random.uniform(jax.random.fold_in(own, position), (shards_of,), jnp.float32, low / len(shards), high / len(shards)))
        level = level * jnp.repeat(draws, shape[position] // shards_of).reshape([-1 if axis == position else 1 for axis in range(len(shape))])
    return level


def scatter_about(stream_key, shape, width, limit, shards=(), kind=jnp.bfloat16):
    gain = block_scale(stream_key, shape, shards, -0.22, 0.18) if shards else 1.0
    drawn = jax.random.normal(stream_key, shape, jnp.float32) * width * gain
    return jnp.minimum(jnp.maximum(drawn, -limit), limit).astype(kind)


def setup_inputs(seed: int = 0) -> dict:
    streams_of = jax.random.split(jax.random.key(seed), 3)
    return {
        "residual": scatter_about(streams_of[0], (NT, 2, NX, NY), 0.15, 0.875, ((0, 64), (2, 4)), jnp.float32),
        "counts": set_ends(jax.random.randint(streams_of[1], (NT,), 1, 5), jax.random.fold_in(streams_of[1], 1), 1, 4).astype(jnp.int32),
    }


phase_rate = 0.004

def signed_wave(indices, length):
    return jnp.where(indices < length // 2, indices, indices - length).astype(jnp.float32)

def reference(residual, counts):
    wave_x = signed_wave(jnp.arange(NX, dtype=jnp.int32), NX)
    wave_y = signed_wave(jnp.arange(NY, dtype=jnp.int32), NY)
    modulus = jnp.sqrt(wave_x[:, None] * wave_x[:, None] + wave_y[None, :] * wave_y[None, :])

    def advance(carried, inputs):
        source, step_count = inputs
        phases = phase_rate * step_count.astype(jnp.float32) * modulus
        cosine = jnp.cos(phases)
        sine_part = jnp.sin(phases)
        spectrum = jnp.fft.fft2(source, axes=(1, 2))
        first_part = cosine * carried[0] + sine_part * carried[1] + spectrum[0]
        second_part = cosine * carried[1] - sine_part * carried[0] + spectrum[1]
        updated = jnp.stack([first_part, second_part])
        physical = jnp.real(jnp.fft.ifft2(updated, axes=(1, 2))).astype(residual.dtype)
        return (updated, physical)
    initial = jnp.zeros_like(jnp.fft.fft2(residual[0], axes=(1, 2)))
    last_state, fields = lax.scan(advance, initial, (residual, counts))
    return fields
```

```python
import functools
import math

import jax
import jax.numpy as jnp
import numpy as np
from jax import lax
from jax.experimental import pallas as pl
from jax.experimental.pallas import tpu as pltpu
from jax.sharding import Mesh
from jax.sharding import PartitionSpec as P

phase_rate = 0.004
F32 = jnp.float32
BF16 = jnp.bfloat16
MESH = pl.DeviceIdType.MESH
LANES = 128
FOLD = 64

SIN_TERMS = [(-1) ** i * math.pi ** (2 * i + 1) / math.factorial(2 * i + 1) for i in range(7)]
COS_TERMS = [(-1) ** i * math.pi ** (2 * i) / math.factorial(2 * i) for i in range(7)]


def cas_tables(length):
    half, quarter = length // 2, length // 4
    place = np.arange(length)
    wave = 2 * (place % half) + place // half
    phases = (np.arange(half)[:, None] * wave[None, :] % length) * (2.0 * math.pi / length)
    table = np.cos(phases) + np.sin(phases)
    table = table.reshape(half, 2, 2, quarter).transpose(1, 2, 0, 3)
    high = table.astype(BF16)
    low = (table - high.astype(np.float64)).astype(BF16)
    return high, low


def halves(x):
    high = x.astype(BF16)
    return high, (x - high.astype(F32)).astype(BF16)


def dot3(a_high, a_low, b_high, b_low):
    dot = functools.partial(jnp.dot, preferred_element_type=F32)
    return dot(a_high, b_high) + (dot(a_low, b_high) + dot(a_high, b_low))


def signed(wave, length):
    return jnp.where(wave < length // 2, wave, wave - length).astype(F32)


def kernel(
    sizes,
    count_ref, source, table_high, table_low, result,
    r, th, tl, xh, xl, sdh, sdl, sa, rb, bh, bl, f0, fs, cosines, sines, zb, tt, ty, ps, pb,
    qh, ql, xs, yb, lh, ll, eo, ob, c_own, c_mate, c_pair, c_z, c_row, c_y,
    load_sem, a_send, a_recv, z_send, z_recv, y_send, y_recv, p_send, p_recv, b_send, b_recv,
    cm_send, cm_recv, cz_send, cz_recv, cy_send, cy_recv, out_sem,
):
    Y, Z, X, N = sizes
    m, H, W, B, XH = N // X, N // 2, N // 4, N // Z, X // 2
    nb = W // B
    yi, zi, ci, xi = (lax.axis_index(a) for a in ("y", "z", "c", "x"))
    mate = 1 - ci
    low_lanes = lax.broadcasted_iota(jnp.int32, (1, LANES), 1) < FOLD

    def swap(x):
        return pltpu.roll(x, FOLD, axis=1)

    def remote(src, dst, send, recv, **where):
        return pltpu.make_async_remote_copy(
            src_ref=src, dst_ref=dst, send_sem=send, recv_sem=recv, device_id=where, device_id_type=MESH
        )

    def x_peers():
        return [(lax.rem(xi + o, X), lax.rem(ci + d, 2)) for o in range(X) for d in range(2) if o or d]

    def z_peers():
        order = sorted(range(1, Z), key=lambda o: -min(o, Z - o))
        return [lax.rem(zi + o, Z) for o in order]

    def chunks(total, rows, body):
        def step(i, carry):
            body(pl.multiple_of(i * rows, rows))
            return carry
        lax.fori_loop(0, total // rows, step, 0)

    def repeat(count, body):
        def step(i, carry):
            body(i)
            return carry
        lax.fori_loop(0, count, step, 0)

    loads = [
        pltpu.make_async_copy(source, r, load_sem.at[0]),
        pltpu.make_async_copy(table_high, th, load_sem.at[1]),
        pltpu.make_async_copy(table_low, tl, load_sem.at[2]),
    ]
    for load in loads:
        load.start()
    c_own[...] = jnp.full(c_own.shape, count_ref[0].astype(F32), F32)

    barrier = pltpu.get_barrier_semaphore()
    for x_to, c_to in x_peers():
        pl.semaphore_signal(barrier, inc=1, device_id={"x": x_to, "c": c_to}, device_id_type=MESH)
    for z_to in z_peers():
        pl.semaphore_signal(barrier, inc=1, device_id={"z": z_to}, device_id_type=MESH)
    for o in range(1, Y):
        pl.semaphore_signal(barrier, inc=1, device_id={"y": lax.rem(yi + o, Y)}, device_id_type=MESH)
    pl.semaphore_wait(barrier, 2 * X - 1 + Z - 1 + Y - 1)

    def to_mate():
        return remote(c_own, c_mate, cm_send, cm_recv, c=mate)

    def pair_to(o):
        return remote(c_pair, c_z.at[o], cz_send.at[o], cz_recv.at[o], z=lax.rem(zi + o, Z))

    def row_to(o):
        return remote(c_row, c_y.at[o], cy_send.at[o], cy_recv.at[o], y=lax.rem(yi + o, Y))

    to_mate().start()

    loads[0].wait()
    for comp in range(2):
        def split_rows(at, comp=comp):
            rows = pl.ds(at, 32)
            first, second = r[comp, rows, :H], r[comp, rows, H:]
            sdh[0, comp, rows, :], sdl[0, comp, rows, :] = halves(first + second)
            sdh[1, comp, rows, :], sdl[1, comp, rows, :] = halves(first - second)
        chunks(m, 32, split_rows)

    to_mate().wait_recv()
    c_pair[...] = c_own[...] + c_mate[...]
    for o in range(1, Z):
        pair_to(o).start()
    loads[1].wait()
    loads[2].wait()

    def a_copy(h, x_to, c_to):
        return remote(sa.at[h, x_to, c_to], rb.at[h, ci, xi], a_send.at[h, x_to, c_to], a_recv.at[h, xi, ci], x=x_to, c=c_to)

    def a_arrival(h, x_from, c_from):
        return remote(sa.at[h, x_from, c_from], rb.at[h, c_from, x_from], a_send.at[h, x_from, c_from],
                      a_recv.at[h, x_from, c_from], x=x_from, c=c_from)

    def along_y(i):
        h, par = i // 2, lax.rem(xi // XH + 1 + i, 2)
        w_part = dot3(sdh[par, 0], sdl[par, 0], th[par, h], tl[par, h])
        v_part = dot3(sdh[par, 1], sdl[par, 1], th[par, h], tl[par, h])
        for k in range(XH):
            x_to = par * XH + k
            wt, vt = w_part[:, k * LANES:(k + 1) * LANES], v_part[:, k * LANES:(k + 1) * LANES]
            sa[h, x_to, 0] = jnp.where(low_lanes, wt, swap(vt))
            sa[h, x_to, 1] = jnp.where(low_lanes, swap(wt), vt)
        for k in range(XH):
            x_to = par * XH + k

            @pl.when(x_to != xi)
            def _():
                a_copy(h, x_to, mate).start()
                a_copy(h, x_to, ci).start()

            @pl.when(x_to == xi)
            def _():
                a_copy(h, x_to, mate).start()
                rb[h, ci, xi] = sa[h, x_to, ci]

    repeat(2, along_y)

    base = jnp.zeros_like(c_own)
    row = c_pair[...]
    for o in range(1, Z):
        pair_to(o).wait_recv()
        row = row + c_z[o]
        base = base + jnp.where(zi >= o, c_z[o], 0.0)
    c_row[...] = row
    for o in range(1, Y):
        row_to(o).start()

    repeat(2, lambda i: along_y(i + 2))

    for par in range(2):
        for h in range(2):
            for k in range(2):
                xh[par, h, k] = th[par, h, k * W:(k + 1) * W, :].astype(F32).T.astype(BF16)
                xl[par, h, k] = tl[par, h, k * W:(k + 1) * W, :].astype(F32).T.astype(BF16)

    for o in range(1, Y):
        row_to(o).wait_recv()
        base = base + jnp.where(yi >= o, c_y[o], 0.0)
    first_count = jnp.where(ci == 0, c_own[...], c_mate[...])
    rates = [
        (base + first_count)[:1] * (phase_rate / math.pi),
        (base + c_pair[...])[:1] * (phase_rate / math.pi),
    ]
    terms = [jnp.where(low_lanes, s, c) for s, c in zip(SIN_TERMS, COS_TERMS)]
    lane = lax.rem(lax.broadcasted_iota(jnp.int32, (1, LANES), 1), FOLD)

    def angles(h):
        col = h * W + lax.rem(xi, XH) * LANES + ci * FOLD + lane
        wave_y = signed(2 * col + xi // XH, N)

        def rows_of(at):
            place = at + lax.broadcasted_iota(jnp.int32, (64, LANES), 0)
            wave_x = signed(2 * lax.rem(place, H) + place // H, N)
            modulus = jnp.sqrt(wave_x * wave_x + wave_y * wave_y)
            for t in range(2):
                turns = modulus * rates[t]
                nearest = jnp.floor(turns + 0.5)
                f = turns - nearest
                g = f * f
                value = terms[-1]
                for term in terms[-2::-1]:
                    value = value * g + term
                value = jnp.where(low_lanes, value * f, value)
                half = nearest * 0.5
                value = jnp.where(half == jnp.floor(half), value, -value)
                other = swap(value)
                cosines[h, t, pl.ds(at, 64), :] = jnp.where(low_lanes, other, value)
                sines[h, t, pl.ds(at, 64), :] = jnp.where(low_lanes, -value, other)
        chunks(N, 64, rows_of)

    repeat(2, angles)

    def z_copy(h, z_to):
        return remote(fs.at[h, pl.ds(pl.multiple_of(z_to * B, B), B)], zb.at[h, zi], z_send.at[h, z_to], z_recv.at[h, zi], z=z_to)

    def z_arrival(h, z_from):
        return remote(zb.at[h, z_from], zb.at[h, z_from], z_send.at[h, z_from], z_recv.at[h, z_from], z=z_from)

    def along_x(h):
        for x_from, c_from in x_peers():
            a_arrival(h, x_from, c_from).wait_recv()
        for k in range(XH):
            for t in range(2):
                def split_rows(at, k=k, t=t):
                    first, second = rb[h, t, k, pl.ds(at, 64), :], rb[h, t, k + XH, pl.ds(at, 64), :]
                    rows = pl.ds(pl.multiple_of(k * m + at, 64), 64)
                    lanes = slice(t * LANES, (t + 1) * LANES)
                    bh[0, rows, lanes], bl[0, rows, lanes] = halves(first + second)
                    bh[1, rows, lanes], bl[1, rows, lanes] = halves(first - second)
                chunks(m, 64, split_rows)

        def quarter(i):
            g = lax.rem(zi // nb + 2 + i, 4)
            par, q = g // 2, lax.rem(g, 2)
            high = jnp.concatenate([xh[par, q, 0], xh[par, q, 1]], axis=1)
            low = jnp.concatenate([xl[par, q, 0], xl[par, q, 1]], axis=1)
            found = dot3(high, low, bh[par], bl[par])
            rows = pl.ds(pl.multiple_of(g * W, W), W)
            z0, z1 = found[:, :LANES], found[:, LANES:]
            framed0 = cosines[h, 0, rows] * z0 + sines[h, 0, rows] * swap(z0)
            framed1 = cosines[h, 1, rows] * z1 + sines[h, 1, rows] * swap(z1)
            f0[h, rows] = framed0
            fs[h, rows] = framed0 + framed1
            for k in range(nb):
                z_to = g * nb + k

                @pl.when(z_to != zi)
                def _():
                    z_copy(h, z_to).start()

                @pl.when(z_to == zi)
                def _():
                    zb[h, zi] = fs[h, pl.ds(pl.multiple_of(z_to * B, B), B)]

        repeat(4, quarter)

    repeat(2, along_x)

    def y_copy(h, o):
        return remote(tt.at[h], ty.at[h, o], y_send.at[h, o], y_recv.at[h, o], y=lax.rem(yi + o, Y))

    def p_copy(h, z_to):
        return remote(ps.at[h, z_to], pb.at[h, zi], p_send.at[h, z_to], p_recv.at[h, zi], z=z_to)

    def p_arrival(h, z_from):
        return remote(ps.at[h, z_from], pb.at[h, z_from], p_send.at[h, z_from], p_recv.at[h, z_from], z=z_from)

    def prefix(h):
        for z_from in z_peers():
            z_arrival(h, z_from).wait_recv()
        total = zb[h, 0]
        for k in range(1, Z):
            total = total + zb[h, k]
        tt[h] = total
        for o in range(1, Y):
            y_copy(h, o).start()
        for o in range(1, Y):
            y_copy(h, o).wait_recv()
        running = jnp.zeros((B, LANES), F32)
        for o in range(1, Y):
            running = running + jnp.where(yi >= o, ty[h, o], 0.0)
        for k in range(Z):
            ps[h, k] = running
            running = running + zb[h, k]
        for z_to in z_peers():
            p_copy(h, z_to).start()
        pb[h, zi] = ps[h, zi]

    repeat(2, prefix)

    def b_copy(h, x_to, t):
        return remote(xs.at[h, x_to, t], yb.at[h, xi, ci], b_send.at[h, x_to, t], b_recv.at[h, xi, ci], x=x_to, c=t)

    def b_arrival(h, x_from, c_from):
        return remote(xs.at[h, x_from, c_from], yb.at[h, x_from, c_from], b_send.at[h, x_from, c_from],
                      b_recv.at[h, x_from, c_from], x=x_from, c=c_from)

    def back_x(h):
        for z_from in z_peers():
            p_arrival(h, z_from).wait_recv()

        def band(k):
            def rows_of(at):
                rows = pl.ds(pl.multiple_of(k * B + at, 64), 64)
                before = pb[h, k, pl.ds(at, 64), :]
                for t, own in ((0, f0), (1, fs)):
                    state = before + own[h, rows, :]
                    state = cosines[h, t, rows, :] * state - sines[h, t, rows, :] * swap(state)
                    lanes = slice(t * LANES, (t + 1) * LANES)
                    qh[rows, lanes], ql[rows, lanes] = halves(state * (1.0 / (N * N)))
            chunks(B, 64, rows_of)

        repeat(Z, band)

        def block(i):
            k = lax.rem(xi + 1 + i, XH)
            rows = pl.ds(pl.multiple_of(k * m, m), m)
            parts = []
            for par in range(2):
                high = jnp.concatenate([th[par, 0, rows], th[par, 1, rows]], axis=1)
                low = jnp.concatenate([tl[par, 0, rows], tl[par, 1, rows]], axis=1)
                waves = slice(par * H, (par + 1) * H)
                parts.append(dot3(high, low, qh[waves, :], ql[waves, :]))
            outs = (parts[0] + parts[1], parts[0] - parts[1])
            for j in range(2):
                for t in range(2):
                    xs[h, k + j * XH, t] = outs[j][:, t * LANES:(t + 1) * LANES]
            for j in range(2):
                x_to = k + j * XH

                @pl.when(x_to != xi)
                def _():
                    b_copy(h, x_to, mate).start()
                    b_copy(h, x_to, ci).start()

                @pl.when(x_to == xi)
                def _():
                    b_copy(h, x_to, mate).start()
                    yb[h, xi, ci] = xs[h, x_to, ci]

        repeat(XH, block)

    repeat(2, back_x)

    def back_y(h, last):
        for x_from, c_from in x_peers():
            b_arrival(h, x_from, c_from).wait_recv()
        for par in range(2):
            for k in range(XH):
                def split_rows(at, par=par, k=k):
                    rows = pl.ds(at, 64)
                    one, two = yb[h, par * XH + k, 0, rows, :], yb[h, par * XH + k, 1, rows, :]
                    lanes = slice(k * LANES, (k + 1) * LANES)
                    lh[par, 0, rows, lanes], ll[par, 0, rows, lanes] = halves(jnp.where(low_lanes, one, swap(two)))
                    lh[par, 1, rows, lanes], ll[par, 1, rows, lanes] = halves(jnp.where(low_lanes, swap(one), two))
                chunks(m, 64, split_rows)

        def component(comp):
            for k in range(2):
                parts = [dot3(lh[par, comp], ll[par, comp], xh[par, h, k], xl[par, h, k]) for par in range(2)]
                if last:
                    even, odd = (eo[comp, k, par] + parts[par] for par in range(2))
                    ob[comp, :, k * W:(k + 1) * W] = even + odd
                    ob[comp, :, H + k * W:H + (k + 1) * W] = even - odd
                else:
                    for par in range(2):
                        eo[comp, k, par] = parts[par]
            if last:
                pltpu.make_async_copy(ob.at[comp], result.at[comp], out_sem.at[comp]).start()

        repeat(2, component)

    back_y(0, False)
    back_y(1, True)

    for comp in range(2):
        pltpu.make_async_copy(ob.at[comp], result.at[comp], out_sem.at[comp]).wait()
    to_mate().wait_send()
    for o in range(1, Z):
        pair_to(o).wait_send()
    for o in range(1, Y):
        row_to(o).wait_send()

    def sent(h):
        for x_to, c_to in x_peers():
            a_copy(h, x_to, c_to).wait_send()
            b_copy(h, x_to, c_to).wait_send()
        for z_to in z_peers():
            z_copy(h, z_to).wait_send()
            p_copy(h, z_to).wait_send()
        for o in range(1, Y):
            y_copy(h, o).wait_send()

    repeat(2, sent)


def call(sizes, residual, counts, high, low):
    Y, Z, X, N = sizes
    m, H, W, B = N // X, N // 2, N // 4, N // Z
    vmem, dma = pltpu.VMEM, pltpu.SemaphoreType.DMA
    anywhere = pl.BlockSpec(memory_space=pl.ANY)
    tile = vmem((8, LANES), F32)
    return pl.pallas_call(
        functools.partial(kernel, sizes),
        out_shape=jax.ShapeDtypeStruct((2, m, N), F32),
        in_specs=[pl.BlockSpec(memory_space=pltpu.SMEM), anywhere, anywhere, anywhere],
        out_specs=anywhere,
        scratch_shapes=[
            vmem((2, m, N), F32),
            vmem((2, 2, H, W), BF16), vmem((2, 2, H, W), BF16),
            vmem((2, 2, 2, W, W), BF16), vmem((2, 2, 2, W, W), BF16),
            vmem((2, 2, m, H), BF16), vmem((2, 2, m, H), BF16),
            vmem((2, X, 2, m, LANES), F32),
            vmem((2, 2, X, m, LANES), F32),
            vmem((2, H, 2 * LANES), BF16), vmem((2, H, 2 * LANES), BF16),
            vmem((2, N, LANES), F32), vmem((2, N, LANES), F32),
            vmem((2, 2, N, LANES), F32), vmem((2, 2, N, LANES), F32),
            vmem((2, Z, B, LANES), F32),
            vmem((2, B, LANES), F32), vmem((2, Y, B, LANES), F32),
            vmem((2, Z, B, LANES), F32), vmem((2, Z, B, LANES), F32),
            vmem((N, 2 * LANES), BF16), vmem((N, 2 * LANES), BF16),
            vmem((2, X, 2, m, LANES), F32), vmem((2, X, 2, m, LANES), F32),
            vmem((2, 2, m, W), BF16), vmem((2, 2, m, W), BF16),
            vmem((2, 2, 2, m, W), F32),
            vmem((2, m, N), F32),
            tile, tile, tile, vmem((Z, 8, LANES), F32), tile, vmem((Y, 8, LANES), F32),
            dma((3,)),
            dma((2, X, 2)), dma((2, X, 2)),
            dma((2, Z)), dma((2, Z)),
            dma((2, Y)), dma((2, Y)),
            dma((2, Z)), dma((2, Z)),
            dma((2, X, 2)), dma((2, X, 2)),
            dma, dma, dma((Z,)), dma((Z,)), dma((Y,)), dma((Y,)),
            dma((2,)),
        ],
        compiler_params=pltpu.CompilerParams(
            collective_id=0, has_side_effects=True, vmem_limit_bytes=60 * 1024 * 1024
        ),
        name="wave",
    )(counts, residual, high, low)


def built(split, length):
    sizes = tuple(split.shape[a] for a in ("y", "z", "x")) + (length,)
    high, low = cas_tables(length)

    def on_device(residual, counts):
        return call(sizes, residual[0], counts, jnp.asarray(high), jnp.asarray(low))[None]

    times = ("y", "z", "c")
    return jax.shard_map(
        on_device,
        mesh=split,
        in_specs=(P(times, None, "x", None), P(times)),
        out_specs=P(times, None, "x", None),
        check_vma=False,
    )


def solution(mesh):
    points, spaces = mesh.shape["tm"], mesh.shape["space"]
    split = Mesh(mesh.devices.reshape(4, points // 8, 2, spaces), ("y", "z", "c", "x"))
    return built(split, 1024)
```

```python
import functools
import math

import jax
import jax.numpy as jnp
import numpy as np
from jax import lax
from jax.experimental import pallas as pl
from jax.experimental.pallas import tpu as pltpu
from jax.sharding import Mesh
from jax.sharding import PartitionSpec as P

phase_rate = 0.004
F32 = jnp.float32
BF16 = jnp.bfloat16
MESH = pl.DeviceIdType.MESH
LANES = 128
FOLD = 32
CHUNKS = 4

SIN_TERMS = [(-1) ** i * math.pi ** (2 * i + 1) / math.factorial(2 * i + 1) for i in range(7)]
COS_TERMS = [(-1) ** i * math.pi ** (2 * i) / math.factorial(2 * i) for i in range(7)]


def cas_tables(length):
    half, quarter = length // 2, length // 4
    place = np.arange(length)
    wave = 2 * (place % half) + place // half
    phases = (np.arange(half)[:, None] * wave[None, :] % length) * (2.0 * math.pi / length)
    table = np.cos(phases) + np.sin(phases)
    table = table.reshape(half, 2, 2, quarter).transpose(1, 2, 0, 3)
    high = table.astype(BF16)
    low = (table - high.astype(np.float64)).astype(BF16)
    return high, low


def halves(x):
    high = x.astype(BF16)
    return high, (x - high.astype(F32)).astype(BF16)


def dot3(a_high, a_low, b_high, b_low):
    dot = functools.partial(jnp.dot, preferred_element_type=F32)
    return dot(a_high, b_high) + (dot(a_low, b_high) + dot(a_high, b_low))


def product(high, low, packed):
    dot = functools.partial(jnp.dot, preferred_element_type=F32)
    both = dot(high, packed)
    return both[:, :LANES] + (both[:, LANES:] + dot(low, packed[:, :LANES]))


def signed(wave, length):
    return jnp.where(wave < length // 2, wave, wave - length).astype(F32)


def kernel(
    sizes,
    count_ref, source, table_high, table_low, result,
    r, th, tl, xh, xl, sdh, sdl, sa, rb, mix, own, fs, cosines, sines, zb, tt, ty, ps, pb,
    q, xs, yb, lh, ll, eo, ob, c_own, c_mate, c_pair, c_z, c_row, c_y,
    load_sem, a_send, a_recv, z_send, z_recv, y_send, y_recv, p_send, p_recv, b_send, b_recv,
    cm_send, cm_recv, cz_send, cz_recv, cy_send, cy_recv, out_sem,
):
    Y, Z, X, N = sizes
    m, H, W, B, XH = N // X, N // 2, N // 4, N // Z, X // 2
    nb, m2, B2 = W // B, m // 2, B // 2
    yi, zi, ci, xi = (lax.axis_index(a) for a in ("y", "z", "c", "x"))
    mate = 1 - ci
    lane = lax.broadcasted_iota(jnp.int32, (1, LANES), 1)
    first_half = lane < 2 * FOLD
    w_lanes = lax.rem(lane, 2 * FOLD) < FOLD

    def turn(x, lanes):
        return pltpu.roll(x, lanes, axis=1)

    def swap(x):
        return jnp.where(w_lanes, turn(x, LANES - FOLD), turn(x, FOLD))

    def cross(a, b):
        return jnp.where(first_half, a, turn(b, 2 * FOLD)), jnp.where(first_half, turn(a, 2 * FOLD), b)

    def weave(a, b):
        return jnp.where(w_lanes, a, turn(b, FOLD)), jnp.where(w_lanes, turn(a, LANES - FOLD), b)

    def remote(src, dst, send, recv, **where):
        return pltpu.make_async_remote_copy(
            src_ref=src, dst_ref=dst, send_sem=send, recv_sem=recv, device_id=where, device_id_type=MESH
        )

    def x_peers():
        return [(lax.rem(xi + o, X), lax.rem(ci + d, 2)) for o in range(X) for d in range(2) if o or d]

    def z_peers():
        order = sorted(range(1, Z), key=lambda o: -min(o, Z - o))
        return [lax.rem(zi + o, Z) for o in order]

    def chunks(total, rows, body):
        def step(i, carry):
            body(pl.multiple_of(i * rows, rows))
            return carry
        lax.fori_loop(0, total // rows, step, 0)

    def repeat(count, body):
        def step(i, carry):
            body(i)
            return carry
        lax.fori_loop(0, count, step, 0)

    loads = [
        pltpu.make_async_copy(source, r, load_sem.at[0]),
        pltpu.make_async_copy(table_high, th, load_sem.at[1]),
        pltpu.make_async_copy(table_low, tl, load_sem.at[2]),
    ]
    for load in loads:
        load.start()
    c_own[...] = jnp.full(c_own.shape, count_ref[0].astype(F32), F32)

    barrier = pltpu.get_barrier_semaphore()
    for x_to, c_to in x_peers():
        pl.semaphore_signal(barrier, inc=1, device_id={"x": x_to, "c": c_to}, device_id_type=MESH)
    for z_to in z_peers():
        pl.semaphore_signal(barrier, inc=1, device_id={"z": z_to}, device_id_type=MESH)
    for o in range(1, Y):
        pl.semaphore_signal(barrier, inc=1, device_id={"y": lax.rem(yi + o, Y)}, device_id_type=MESH)
    pl.semaphore_wait(barrier, 2 * X - 1 + Z - 1 + Y - 1)

    def to_mate():
        return remote(c_own, c_mate, cm_send, cm_recv, c=mate)

    def pair_to(o):
        return remote(c_pair, c_z.at[o], cz_send.at[o], cz_recv.at[o], z=lax.rem(zi + o, Z))

    def row_to(o):
        return remote(c_row, c_y.at[o], cy_send.at[o], cy_recv.at[o], y=lax.rem(yi + o, Y))

    to_mate().start()

    loads[0].wait()
    for comp in range(2):
        def split_rows(at, comp=comp):
            rows = pl.ds(at, 32)
            first, second = r[comp, rows, :H], r[comp, rows, H:]
            sdh[0, comp, rows, :], sdl[0, comp, rows, :] = halves(first + second)
            sdh[1, comp, rows, :], sdl[1, comp, rows, :] = halves(first - second)
        chunks(m, 32, split_rows)

    loads[1].wait()
    loads[2].wait()

    def a_copy(h, x_to, c_to):
        return remote(sa.at[h, x_to, c_to], rb.at[h, ci, xi], a_send.at[h, x_to, c_to], a_recv.at[h, xi, ci], x=x_to, c=c_to)

    def a_arrival(h, x_from, c_from):
        return remote(sa.at[h, x_from, c_from], rb.at[h, c_from, x_from], a_send.at[h, x_from, c_from],
                      a_recv.at[h, x_from, c_from], x=x_from, c=c_from)

    def along_y(i):
        pair, par = i // 2, lax.rem(xi // XH + 1 + i, 2)
        w_part = dot3(sdh[par, 0], sdl[par, 0], th[par, pair], tl[par, pair])
        v_part = dot3(sdh[par, 1], sdl[par, 1], th[par, pair], tl[par, pair])
        for j in range(2):
            lanes = slice(j * LANES, (j + 1) * LANES)
            w_tiles = cross(w_part[:m2, lanes], w_part[m2:, lanes])
            v_tiles = cross(v_part[:m2, lanes], v_part[m2:, lanes])
            for k in range(XH):
                sa[2 * pair + j, par * XH + k, 0], sa[2 * pair + j, par * XH + k, 1] = weave(w_tiles[k], v_tiles[k])

    def send_along_y(h, q):
        par = lax.rem(xi // XH + 1 + q, 2)
        for k in range(XH):
            x_to = par * XH + k

            @pl.when(x_to != xi)
            def _():
                a_copy(h, x_to, mate).start()
                a_copy(h, x_to, ci).start()

            @pl.when(x_to == xi)
            def _():
                a_copy(h, x_to, mate).start()
                rb[h, ci, xi] = sa[h, x_to, ci]

    def first_stage(pair):
        along_y(2 * pair)
        send_along_y(2 * pair, 0)
        along_y(2 * pair + 1)
        send_along_y(2 * pair, 1)
        send_along_y(2 * pair + 1, 0)
        send_along_y(2 * pair + 1, 1)

    first_stage(0)
    to_mate().wait_recv()
    c_pair[...] = c_own[...] + c_mate[...]
    for o in range(1, Z):
        pair_to(o).start()
    first_stage(1)

    base = jnp.zeros_like(c_own)
    row = c_pair[...]
    for o in range(1, Z):
        pair_to(o).wait_recv()
        row = row + c_z[o]
        base = base + jnp.where(zi >= o, c_z[o], 0.0)
    c_row[...] = row
    for o in range(1, Y):
        row_to(o).start()

    for par in range(2):
        for h in range(2):
            for k in range(2):
                xh[par, h, k] = th[par, h, k * W:(k + 1) * W, :].astype(F32).T.astype(BF16)
                xl[par, h, k] = tl[par, h, k * W:(k + 1) * W, :].astype(F32).T.astype(BF16)

    for o in range(1, Y):
        row_to(o).wait_recv()
        base = base + jnp.where(yi >= o, c_y[o], 0.0)
    first_count = jnp.where(ci == 0, c_own[...], c_mate[...])
    rates = jnp.where(first_half, (base + first_count)[:1], (base + c_pair[...])[:1]) * (phase_rate / math.pi)
    terms = [jnp.where(w_lanes, s, c) for s, c in zip(SIN_TERMS, COS_TERMS)]
    column = lax.rem(lane, FOLD)

    def angles(h):
        col = h * LANES + lax.rem(xi, XH) * 2 * FOLD + ci * FOLD + column
        wave_y = signed(2 * col + xi // XH, N)

        def rows_of(at):
            place = at + lax.broadcasted_iota(jnp.int32, (64, LANES), 0)
            wave_x = signed(2 * lax.rem(place, H) + place // H, N)
            turns = jnp.sqrt(wave_x * wave_x + wave_y * wave_y) * rates
            nearest = jnp.floor(turns + 0.5)
            f = turns - nearest
            g = f * f
            value = terms[-1]
            for term in terms[-2::-1]:
                value = value * g + term
            value = jnp.where(w_lanes, value * f, value)
            half = nearest * 0.5
            value = jnp.where(half == jnp.floor(half), value, -value)
            other = swap(value)
            cosines[h, pl.ds(at, 64), :] = jnp.where(w_lanes, other, value)
            sines[h, pl.ds(at, 64), :] = jnp.where(w_lanes, -value, other)
        chunks(N, 64, rows_of)

    def z_copy(h, z_to):
        return remote(fs.at[h, z_to], zb.at[h, zi], z_send.at[h, z_to], z_recv.at[h, zi], z=z_to)

    def z_arrival(h, z_from):
        return remote(zb.at[h, z_from], zb.at[h, z_from], z_send.at[h, z_from], z_recv.at[h, z_from], z=z_from)

    def along_x(h):
        for x_from, c_from in x_peers():
            a_arrival(h, x_from, c_from).wait_recv()
        for k in range(XH):
            def split_rows(at, k=k):
                def place(par, half, x):
                    rows = pl.ds(pl.multiple_of(k * m + half * m2 + at, 64), 64)
                    mix[par, rows, :LANES], mix[par, rows, LANES:] = halves(x)
                near = [rb[h, t, k, pl.ds(at, 64), :] for t in range(2)]
                far = [rb[h, t, k + XH, pl.ds(at, 64), :] for t in range(2)]
                for half, x in enumerate(cross(near[0] + far[0], near[1] + far[1])):
                    place(0, half, x)
                for half, x in enumerate(cross(near[0] - far[0], near[1] - far[1])):
                    place(1, half, x)
            chunks(m2, 64, split_rows)

        def quarter(i):
            g = lax.rem(zi // nb + 2 + i, 4)
            par, half = g // 2, lax.rem(g, 2)
            high = jnp.concatenate([xh[par, half, 0], xh[par, half, 1]], axis=1)
            low = jnp.concatenate([xl[par, half, 0], xl[par, half, 1]], axis=1)
            found = product(high, low, mix[par])
            rows = pl.ds(pl.multiple_of(g * W, W), W)
            framed = cosines[h, rows] * found + sines[h, rows] * swap(found)
            framed = framed + jnp.where(first_half, 0.0, turn(framed, 2 * FOLD))
            own[h, rows] = framed
            for k in range(nb):
                z_to = g * nb + k
                a, b = framed[k * B:k * B + B2], framed[k * B + B2:(k + 1) * B]
                fs[h, z_to] = jnp.where(first_half, turn(a, 2 * FOLD), b)
            for k in range(nb):
                z_to = g * nb + k

                @pl.when(z_to != zi)
                def _():
                    z_copy(h, z_to).start()

                @pl.when(z_to == zi)
                def _():
                    zb[h, zi] = fs[h, zi]

        repeat(4, quarter)

    def y_copy(h, o):
        return remote(tt.at[h], ty.at[h, o], y_send.at[h, o], y_recv.at[h, o], y=lax.rem(yi + o, Y))

    def p_copy(h, z_to):
        return remote(ps.at[h, z_to], pb.at[h, zi], p_send.at[h, z_to], p_recv.at[h, zi], z=z_to)

    def p_arrival(h, z_from):
        return remote(ps.at[h, z_from], pb.at[h, z_from], p_send.at[h, z_from], p_recv.at[h, z_from], z=z_from)

    def totals(h):
        for z_from in z_peers():
            z_arrival(h, z_from).wait_recv()
        total = zb[h, 0]
        for k in range(1, Z):
            total = total + zb[h, k]
        tt[h] = total
        for o in range(1, Y):
            y_copy(h, o).start()

    def prefix(h):
        for o in range(1, Y):
            y_copy(h, o).wait_recv()
        running = jnp.zeros((B2, LANES), F32)
        for o in range(1, Y):
            running = running + jnp.where(yi >= o, ty[h, o], 0.0)
        for k in range(Z):
            ps[h, k] = running
            running = running + zb[h, k]
        for z_to in z_peers():
            p_copy(h, z_to).start()
        pb[h, zi] = ps[h, zi]

    def forward(i):
        angles(i)
        along_x(i)

    repeat(3, forward)
    totals(0)
    forward(3)

    def middle(i):
        totals(i + 1)
        prefix(i)

    repeat(3, middle)
    prefix(3)

    def b_copy(h, x_to, t):
        return remote(xs.at[h, x_to, t], yb.at[h, xi, ci], b_send.at[h, x_to, t], b_recv.at[h, xi, ci], x=x_to, c=t)

    def b_arrival(h, x_from, c_from):
        return remote(xs.at[h, x_from, c_from], yb.at[h, x_from, c_from], b_send.at[h, x_from, c_from],
                      b_recv.at[h, x_from, c_from], x=x_from, c=c_from)

    def back_x(h):
        for z_from in z_peers():
            p_arrival(h, z_from).wait_recv()

        def band(k):
            before = pb[h, k]
            for half, x in enumerate(cross(before, before)):
                rows = pl.ds(pl.multiple_of(k * B + half * B2, B2), B2)
                state = x + own[h, rows, :]
                state = cosines[h, rows, :] * state - sines[h, rows, :] * swap(state)
                q[rows, :LANES], q[rows, LANES:] = halves(state)

        repeat(Z, band)

        def block(i):
            k = lax.rem(xi + 1 + i, XH)
            rows = pl.ds(pl.multiple_of(k * m, m), m)
            parts = []
            for par in range(2):
                high = jnp.concatenate([th[par, 0, rows], th[par, 1, rows]], axis=1)
                low = jnp.concatenate([tl[par, 0, rows], tl[par, 1, rows]], axis=1)
                parts.append(product(high, low, q[par * H:(par + 1) * H]))
            for j, out in enumerate((parts[0] + parts[1], parts[0] - parts[1])):
                xs[h, k + j * XH, 0], xs[h, k + j * XH, 1] = cross(out[:m2], out[m2:])
            for j in range(2):
                x_to = k + j * XH

                @pl.when(x_to != xi)
                def _():
                    b_copy(h, x_to, mate).start()
                    b_copy(h, x_to, ci).start()

                @pl.when(x_to == xi)
                def _():
                    b_copy(h, x_to, mate).start()
                    yb[h, xi, ci] = xs[h, x_to, ci]

        repeat(XH, block)

    repeat(CHUNKS, back_x)

    def back_y(pair, last):
        for j in range(2):
            for x_from, c_from in x_peers():
                b_arrival(2 * pair + j, x_from, c_from).wait_recv()
        for par in range(2):
            for j in range(2):
                def split_rows(at, par=par, j=j):
                    tiles = [weave(yb[2 * pair + j, par * XH + k, 0, pl.ds(at, 64), :],
                                   yb[2 * pair + j, par * XH + k, 1, pl.ds(at, 64), :]) for k in range(XH)]
                    lanes = slice(j * LANES, (j + 1) * LANES)
                    for comp in range(2):
                        for half, x in enumerate(cross(tiles[0][comp], tiles[1][comp])):
                            rows = pl.ds(pl.multiple_of(half * m2 + at, 64), 64)
                            lh[par, comp, rows, lanes], ll[par, comp, rows, lanes] = halves(x)
                chunks(m2, 64, split_rows)

        def component(comp):
            for k in range(2):
                parts = [dot3(lh[par, comp], ll[par, comp], xh[par, pair, k], xl[par, pair, k]) for par in range(2)]
                if last:
                    even, odd = (eo[comp, k, par] + parts[par] for par in range(2))
                    ob[comp, :, k * W:(k + 1) * W] = even + odd
                    ob[comp, :, H + k * W:H + (k + 1) * W] = even - odd
                else:
                    for par in range(2):
                        eo[comp, k, par] = parts[par]
            if last:
                pltpu.make_async_copy(ob.at[comp], result.at[comp], out_sem.at[comp]).start()

        repeat(2, component)

    back_y(0, False)
    back_y(1, True)

    for comp in range(2):
        pltpu.make_async_copy(ob.at[comp], result.at[comp], out_sem.at[comp]).wait()
    to_mate().wait_send()
    for o in range(1, Z):
        pair_to(o).wait_send()
    for o in range(1, Y):
        row_to(o).wait_send()

    def sent(h):
        for x_to, c_to in x_peers():
            a_copy(h, x_to, c_to).wait_send()
            b_copy(h, x_to, c_to).wait_send()
        for z_to in z_peers():
            z_copy(h, z_to).wait_send()
            p_copy(h, z_to).wait_send()
        for o in range(1, Y):
            y_copy(h, o).wait_send()

    repeat(CHUNKS, sent)


def call(sizes, residual, counts, high, low):
    Y, Z, X, N = sizes
    m, H, W, B = N // X, N // 2, N // 4, N // Z
    vmem, dma = pltpu.VMEM, pltpu.SemaphoreType.DMA
    anywhere = pl.BlockSpec(memory_space=pl.ANY)
    tile = vmem((8, LANES), F32)
    return pl.pallas_call(
        functools.partial(kernel, sizes),
        out_shape=jax.ShapeDtypeStruct((2, m, N), F32),
        in_specs=[pl.BlockSpec(memory_space=pltpu.SMEM), anywhere, anywhere, anywhere],
        out_specs=anywhere,
        scratch_shapes=[
            vmem((2, m, N), F32),
            vmem((2, 2, H, W), BF16), vmem((2, 2, H, W), BF16),
            vmem((2, 2, 2, W, W), BF16), vmem((2, 2, 2, W, W), BF16),
            vmem((2, 2, m, H), BF16), vmem((2, 2, m, H), BF16),
            vmem((CHUNKS, X, 2, m // 2, LANES), F32),
            vmem((CHUNKS, 2, X, m // 2, LANES), F32),
            vmem((2, H, 2 * LANES), BF16),
            vmem((CHUNKS, N, LANES), F32),
            vmem((CHUNKS, Z, B // 2, LANES), F32),
            vmem((CHUNKS, N, LANES), F32), vmem((CHUNKS, N, LANES), F32),
            vmem((CHUNKS, Z, B // 2, LANES), F32),
            vmem((CHUNKS, B // 2, LANES), F32), vmem((CHUNKS, Y, B // 2, LANES), F32),
            vmem((CHUNKS, Z, B // 2, LANES), F32), vmem((CHUNKS, Z, B // 2, LANES), F32),
            vmem((N, 2 * LANES), BF16),
            vmem((CHUNKS, X, 2, m // 2, LANES), F32), vmem((CHUNKS, X, 2, m // 2, LANES), F32),
            vmem((2, 2, m, W), BF16), vmem((2, 2, m, W), BF16),
            vmem((2, 2, 2, m, W), F32),
            vmem((2, m, N), F32),
            tile, tile, tile, vmem((Z, 8, LANES), F32), tile, vmem((Y, 8, LANES), F32),
            dma((3,)),
            dma((CHUNKS, X, 2)), dma((CHUNKS, X, 2)),
            dma((CHUNKS, Z)), dma((CHUNKS, Z)),
            dma((CHUNKS, Y)), dma((CHUNKS, Y)),
            dma((CHUNKS, Z)), dma((CHUNKS, Z)),
            dma((CHUNKS, X, 2)), dma((CHUNKS, X, 2)),
            dma, dma, dma((Z,)), dma((Z,)), dma((Y,)), dma((Y,)),
            dma((2,)),
        ],
        compiler_params=pltpu.CompilerParams(
            collective_id=0, has_side_effects=True, vmem_limit_bytes=60 * 1024 * 1024
        ),
        name="wave",
    )(counts, residual, high, low)


def built(split, length):
    sizes = tuple(split.shape[a] for a in ("y", "z", "x")) + (length,)
    high, low = cas_tables(length)

    def on_device(residual, counts):
        return call(sizes, residual[0], counts, jnp.asarray(high), jnp.asarray(low))[None] * (1.0 / (length * length))

    times = ("y", "z", "c")
    return jax.shard_map(
        on_device,
        mesh=split,
        in_specs=(P(times, None, "x", None), P(times)),
        out_specs=P(times, None, "x", None),
        check_vma=False,
    )


def solution(mesh):
    points, spaces = mesh.shape["tm"], mesh.shape["space"]
    split = Mesh(mesh.devices.reshape(4, points // 8, 2, spaces), ("y", "z", "c", "x"))
    return built(split, 1024)
```

```python
import functools
import math

import jax
import jax.numpy as jnp
import numpy as np
from jax import lax
from jax.experimental import pallas as pl
from jax.experimental.pallas import tpu as pltpu
from jax.sharding import Mesh
from jax.sharding import PartitionSpec as P

phase_rate = 0.004
F32 = jnp.float32
BF16 = jnp.bfloat16
MESH = pl.DeviceIdType.MESH
LANES = 128
FOLD = 32
CHUNKS = 4

SIN_TERMS = [(-1) ** i * math.pi ** (2 * i + 1) / math.factorial(2 * i + 1) for i in range(7)]
COS_TERMS = [(-1) ** i * math.pi ** (2 * i) / math.factorial(2 * i) for i in range(7)]


def cas_tables(length):
    half, quarter = length // 2, length // 4
    place = np.arange(length)
    wave = 2 * (place % half) + place // half
    phases = (np.arange(half)[:, None] * wave[None, :] % length) * (2.0 * math.pi / length)
    table = np.cos(phases) + np.sin(phases)
    table = table.reshape(half, 2, 2, quarter).transpose(1, 2, 0, 3)
    high = table.astype(BF16)
    low = (table - high.astype(np.float64)).astype(BF16)
    return high, low


def halves(x):
    high = x.astype(BF16)
    return high, (x - high.astype(F32)).astype(BF16)


def dot3(a_high, a_low, b_high, b_low):
    dot = functools.partial(jnp.dot, preferred_element_type=F32)
    return dot(a_high, b_high) + (dot(a_low, b_high) + dot(a_high, b_low))


def product(high, low, packed):
    dot = functools.partial(jnp.dot, preferred_element_type=F32)
    both = dot(high, packed)
    return both[:, :LANES] + (both[:, LANES:] + dot(low, packed[:, :LANES]))


def signed(wave, length):
    return jnp.where(wave < length // 2, wave, wave - length).astype(F32)


def kernel(
    sizes,
    count_ref, source, table_high, table_low, result,
    r, th, tl, xh, xl, sdh, sdl, sa, rb, mix, own, fs, cosines, sines, zb, tt, ty, ps, pb,
    q, xs, yb, lh, ll, eo, c_own, c_mate, c_pair, c_z, c_row, c_y,
    load_sem, a_send, a_recv, z_send, z_recv, y_send, y_recv, p_send, p_recv, b_send, b_recv,
    cm_send, cm_recv, cz_send, cz_recv, cy_send, cy_recv, ready, go,
):
    Y, Z, X, N = sizes
    m, H, W, B, XH = N // X, N // 2, N // 4, N // Z, X // 2
    nb, m2, B2 = W // B, m // 2, B // 2
    yi, zi, ci, xi = (lax.axis_index(a) for a in ("y", "z", "c", "x"))
    mate = 1 - ci
    lane = lax.broadcasted_iota(jnp.int32, (1, LANES), 1)
    first_half = lane < 2 * FOLD
    w_lanes = lax.rem(lane, 2 * FOLD) < FOLD

    def turn(x, lanes):
        return pltpu.roll(x, lanes, axis=1)

    def swap(x):
        return jnp.where(w_lanes, turn(x, LANES - FOLD), turn(x, FOLD))

    def cross(a, b):
        return jnp.where(first_half, a, turn(b, 2 * FOLD)), jnp.where(first_half, turn(a, 2 * FOLD), b)

    def weave(a, b):
        return jnp.where(w_lanes, a, turn(b, FOLD)), jnp.where(w_lanes, turn(a, LANES - FOLD), b)

    def remote(src, dst, send, recv, **where):
        return pltpu.make_async_remote_copy(
            src_ref=src, dst_ref=dst, send_sem=send, recv_sem=recv, device_id=where, device_id_type=MESH
        )

    def x_peers():
        return [(lax.rem(xi + o, X), lax.rem(ci + d, 2)) for o in range(X) for d in range(2) if o or d]

    def z_peers():
        order = sorted(range(1, Z), key=lambda o: -min(o, Z - o))
        return [lax.rem(zi + o, Z) for o in order]

    def chunks(total, rows, body):
        def step(i, carry):
            body(pl.multiple_of(i * rows, rows))
            return carry
        lax.fori_loop(0, total // rows, step, 0)

    def repeat(count, body):
        def step(i, carry):
            body(i)
            return carry
        lax.fori_loop(0, count, step, 0)

    loads = [
        pltpu.make_async_copy(source, r, load_sem.at[0]),
        pltpu.make_async_copy(table_high, th, load_sem.at[1]),
        pltpu.make_async_copy(table_low, tl, load_sem.at[2]),
    ]
    for load in loads:
        load.start()

    barrier = pltpu.get_barrier_semaphore()
    lead = jnp.logical_and(xi == 0, ci == 1)
    for x_to, c_to in x_peers():
        @pl.when(jnp.logical_not(jnp.logical_and(x_to == 0, c_to == 1)))
        def _():
            pl.semaphore_signal(barrier, inc=1, device_id={"x": x_to, "c": c_to}, device_id_type=MESH)

    def group_is_here():
        @pl.when(jnp.logical_not(lead))
        def _():
            pl.semaphore_wait(barrier, 2 * X - 1)

        @pl.when(jnp.logical_and(xi == 0, ci == 0))
        def _():
            pl.semaphore_signal(ready, inc=1, device_id={"c": mate}, device_id_type=MESH)

        @pl.when(lead)
        def _():
            pl.semaphore_wait(ready, 1)
            for z_to in z_peers():
                pl.semaphore_signal(barrier, inc=1, device_id={"z": z_to}, device_id_type=MESH)
            for o in range(1, Y):
                pl.semaphore_signal(barrier, inc=1, device_id={"y": lax.rem(yi + o, Y)}, device_id_type=MESH)

    def all_are_here():
        @pl.when(lead)
        def _():
            pl.semaphore_wait(barrier, Z - 1 + Y - 1)
            for x_to, c_to in x_peers():
                pl.semaphore_signal(go, inc=1, device_id={"x": x_to, "c": c_to}, device_id_type=MESH)

        @pl.when(jnp.logical_not(lead))
        def _():
            pl.semaphore_wait(go, 1)

    def to_mate():
        return remote(c_own, c_mate, cm_send, cm_recv, c=mate)

    def pair_to(o):
        return remote(c_pair, c_z.at[o], cz_send.at[o], cz_recv.at[o], z=lax.rem(zi + o, Z))

    def row_to(o):
        return remote(c_row, c_y.at[o], cy_send.at[o], cy_recv.at[o], y=lax.rem(yi + o, Y))

    loads[0].wait()
    for comp in range(2):
        def split_rows(at, comp=comp):
            rows = pl.ds(at, 32)
            first, second = r[comp, rows, :H], r[comp, rows, H:]
            sdh[0, comp, rows, :], sdl[0, comp, rows, :] = halves(first + second)
            sdh[1, comp, rows, :], sdl[1, comp, rows, :] = halves(first - second)
        chunks(m, 32, split_rows)

    loads[1].wait()
    loads[2].wait()

    def a_copy(h, x_to, c_to):
        return remote(sa.at[h, x_to, c_to], rb.at[h, ci, xi], a_send.at[h, x_to, c_to], a_recv.at[h, xi, ci], x=x_to, c=c_to)

    def a_arrival(h, x_from, c_from):
        return remote(sa.at[h, x_from, c_from], rb.at[h, c_from, x_from], a_send.at[h, x_from, c_from],
                      a_recv.at[h, x_from, c_from], x=x_from, c=c_from)

    def along_y(i):
        pair, par = i // 2, lax.rem(xi // XH + 1 + i, 2)
        w_part = dot3(sdh[par, 0], sdl[par, 0], th[par, pair], tl[par, pair])
        v_part = dot3(sdh[par, 1], sdl[par, 1], th[par, pair], tl[par, pair])
        for j in range(2):
            lanes = slice(j * LANES, (j + 1) * LANES)
            w_tiles = cross(w_part[:m2, lanes], w_part[m2:, lanes])
            v_tiles = cross(v_part[:m2, lanes], v_part[m2:, lanes])
            for k in range(XH):
                sa[2 * pair + j, par * XH + k, 0], sa[2 * pair + j, par * XH + k, 1] = weave(w_tiles[k], v_tiles[k])

    def send_along_y(h, q):
        par = lax.rem(xi // XH + 1 + q, 2)
        for k in range(XH):
            x_to = par * XH + k

            @pl.when(x_to != xi)
            def _():
                a_copy(h, x_to, mate).start()
                a_copy(h, x_to, ci).start()

            @pl.when(x_to == xi)
            def _():
                a_copy(h, x_to, mate).start()
                rb[h, ci, xi] = sa[h, x_to, ci]

    c_own[...] = jnp.full(c_own.shape, count_ref[0].astype(F32), F32)
    along_y(0)
    group_is_here()
    to_mate().start()
    send_along_y(0, 0)
    along_y(1)
    for h, side in ((0, 1), (1, 0), (1, 1)):
        send_along_y(h, side)
    all_are_here()
    to_mate().wait_recv()
    c_pair[...] = c_own[...] + c_mate[...]
    for o in range(1, Z):
        pair_to(o).start()
    for side in range(2):
        along_y(2 + side)
    for h in (2, 3):
        for side in range(2):
            send_along_y(h, side)

    base = jnp.zeros_like(c_own)
    row = c_pair[...]
    for o in range(1, Z):
        pair_to(o).wait_recv()
        row = row + c_z[o]
        base = base + jnp.where(zi >= o, c_z[o], 0.0)
    c_row[...] = row
    for o in range(1, Y):
        row_to(o).start()

    for par in range(2):
        for h in range(2):
            for k in range(2):
                xh[par, h, k] = th[par, h, k * W:(k + 1) * W, :].astype(F32).T.astype(BF16)
                xl[par, h, k] = tl[par, h, k * W:(k + 1) * W, :].astype(F32).T.astype(BF16)

    for o in range(1, Y):
        row_to(o).wait_recv()
        base = base + jnp.where(yi >= o, c_y[o], 0.0)
    first_count = jnp.where(ci == 0, c_own[...], c_mate[...])
    rates = jnp.where(first_half, (base + first_count)[:1], (base + c_pair[...])[:1]) * (phase_rate / math.pi)
    terms = [jnp.where(w_lanes, s, c) for s, c in zip(SIN_TERMS, COS_TERMS)]
    column = lax.rem(lane, FOLD)

    def angles(h):
        col = h * LANES + lax.rem(xi, XH) * 2 * FOLD + ci * FOLD + column
        wave_y = signed(2 * col + xi // XH, N)

        def rows_of(at):
            place = at + lax.broadcasted_iota(jnp.int32, (64, LANES), 0)
            wave_x = signed(2 * lax.rem(place, H) + place // H, N)
            turns = jnp.sqrt(wave_x * wave_x + wave_y * wave_y) * rates
            nearest = jnp.floor(turns + 0.5)
            f = turns - nearest
            g = f * f
            value = terms[-1]
            for term in terms[-2::-1]:
                value = value * g + term
            value = jnp.where(w_lanes, value * f, value)
            half = nearest * 0.5
            value = jnp.where(half == jnp.floor(half), value, -value)
            other = swap(value)
            cosines[h, pl.ds(at, 64), :] = jnp.where(w_lanes, other, value)
            sines[h, pl.ds(at, 64), :] = jnp.where(w_lanes, -value, other)
        chunks(N, 64, rows_of)

    def z_copy(h, z_to):
        return remote(fs.at[h, z_to], zb.at[h, zi], z_send.at[h, z_to], z_recv.at[h, zi], z=z_to)

    def z_arrival(h, z_from):
        return remote(zb.at[h, z_from], zb.at[h, z_from], z_send.at[h, z_from], z_recv.at[h, z_from], z=z_from)

    def along_x(h):
        for x_from, c_from in x_peers():
            a_arrival(h, x_from, c_from).wait_recv()
        for k in range(XH):
            def split_rows(at, k=k):
                def place(par, half, x):
                    rows = pl.ds(pl.multiple_of(k * m + half * m2 + at, 64), 64)
                    mix[par, rows, :LANES], mix[par, rows, LANES:] = halves(x)
                near = [rb[h, t, k, pl.ds(at, 64), :] for t in range(2)]
                far = [rb[h, t, k + XH, pl.ds(at, 64), :] for t in range(2)]
                for half, x in enumerate(cross(near[0] + far[0], near[1] + far[1])):
                    place(0, half, x)
                for half, x in enumerate(cross(near[0] - far[0], near[1] - far[1])):
                    place(1, half, x)
            chunks(m2, 64, split_rows)

        def quarter(i):
            g = lax.rem(zi // nb + 2 + i, 4)
            par, half = g // 2, lax.rem(g, 2)
            high = jnp.concatenate([xh[par, half, 0], xh[par, half, 1]], axis=1)
            low = jnp.concatenate([xl[par, half, 0], xl[par, half, 1]], axis=1)
            found = product(high, low, mix[par])
            rows = pl.ds(pl.multiple_of(g * W, W), W)
            framed = cosines[h, rows] * found + sines[h, rows] * swap(found)
            framed = framed + jnp.where(first_half, 0.0, turn(framed, 2 * FOLD))
            own[h, rows] = framed
            for k in range(nb):
                z_to = g * nb + k
                a, b = framed[k * B:k * B + B2], framed[k * B + B2:(k + 1) * B]
                fs[h, z_to] = jnp.where(first_half, turn(a, 2 * FOLD), b)
            for k in range(nb):
                z_to = g * nb + k

                @pl.when(z_to != zi)
                def _():
                    z_copy(h, z_to).start()

                @pl.when(z_to == zi)
                def _():
                    zb[h, zi] = fs[h, zi]

        repeat(4, quarter)

    def y_copy(h, o):
        return remote(tt.at[h], ty.at[h, o], y_send.at[h, o], y_recv.at[h, o], y=lax.rem(yi + o, Y))

    def p_copy(h, z_to):
        return remote(ps.at[h, z_to], pb.at[h, zi], p_send.at[h, z_to], p_recv.at[h, zi], z=z_to)

    def p_arrival(h, z_from):
        return remote(ps.at[h, z_from], pb.at[h, z_from], p_send.at[h, z_from], p_recv.at[h, z_from], z=z_from)

    def totals(h):
        for z_from in z_peers():
            z_arrival(h, z_from).wait_recv()
        total = zb[h, 0]
        for k in range(1, Z):
            total = total + zb[h, k]
        tt[h] = total
        for o in range(1, Y):
            y_copy(h, o).start()

    def prefix(h):
        for o in range(1, Y):
            y_copy(h, o).wait_recv()
        running = jnp.zeros((B2, LANES), F32)
        for o in range(1, Y):
            running = running + jnp.where(yi >= o, ty[h, o], 0.0)
        for k in range(Z):
            ps[h, k] = running
            running = running + zb[h, k]
        for z_to in z_peers():
            p_copy(h, z_to).start()
        pb[h, zi] = ps[h, zi]

    def forward(i):
        angles(i)
        along_x(i)

    repeat(3, forward)
    totals(0)
    forward(3)

    def middle(i):
        totals(i + 1)
        prefix(i)

    repeat(3, middle)
    prefix(3)

    def b_copy(h, x_to, t):
        return remote(xs.at[h, x_to, t], yb.at[h, xi, ci], b_send.at[h, x_to, t], b_recv.at[h, xi, ci], x=x_to, c=t)

    def b_arrival(h, x_from, c_from):
        return remote(xs.at[h, x_from, c_from], yb.at[h, x_from, c_from], b_send.at[h, x_from, c_from],
                      b_recv.at[h, x_from, c_from], x=x_from, c=c_from)

    def back_x(h):
        for z_from in z_peers():
            p_arrival(h, z_from).wait_recv()

        def band(k):
            before = pb[h, k]
            for half, x in enumerate(cross(before, before)):
                rows = pl.ds(pl.multiple_of(k * B + half * B2, B2), B2)
                state = x + own[h, rows, :]
                state = cosines[h, rows, :] * state - sines[h, rows, :] * swap(state)
                q[rows, :LANES], q[rows, LANES:] = halves(state * (1.0 / (N * N)))

        repeat(Z, band)

        def block(i):
            k = lax.rem(xi + 1 + i, XH)
            rows = pl.ds(pl.multiple_of(k * m, m), m)
            parts = []
            for par in range(2):
                high = jnp.concatenate([th[par, 0, rows], th[par, 1, rows]], axis=1)
                low = jnp.concatenate([tl[par, 0, rows], tl[par, 1, rows]], axis=1)
                parts.append(product(high, low, q[par * H:(par + 1) * H]))
            for j, out in enumerate((parts[0] + parts[1], parts[0] - parts[1])):
                xs[h, k + j * XH, 0], xs[h, k + j * XH, 1] = cross(out[:m2], out[m2:])
            for j in range(2):
                x_to = k + j * XH

                @pl.when(x_to != xi)
                def _():
                    b_copy(h, x_to, mate).start()
                    b_copy(h, x_to, ci).start()

                @pl.when(x_to == xi)
                def _():
                    b_copy(h, x_to, mate).start()
                    yb[h, xi, ci] = xs[h, x_to, ci]

        repeat(XH, block)

    repeat(CHUNKS, back_x)

    def back_y(pair, last):
        for j in range(2):
            for x_from, c_from in x_peers():
                b_arrival(2 * pair + j, x_from, c_from).wait_recv()
            for par in range(2):
                def split_rows(at, par=par, j=j):
                    tiles = [weave(yb[2 * pair + j, par * XH + k, 0, pl.ds(at, 64), :],
                                   yb[2 * pair + j, par * XH + k, 1, pl.ds(at, 64), :]) for k in range(XH)]
                    lanes = slice(j * LANES, (j + 1) * LANES)
                    for comp in range(2):
                        for half, x in enumerate(cross(tiles[0][comp], tiles[1][comp])):
                            rows = pl.ds(pl.multiple_of(half * m2 + at, 64), 64)
                            lh[par, comp, rows, lanes], ll[par, comp, rows, lanes] = halves(x)
                chunks(m2, 64, split_rows)

        def component(comp):
            for k in range(2):
                parts = [dot3(lh[par, comp], ll[par, comp], xh[par, pair, k], xl[par, pair, k]) for par in range(2)]
                if last:
                    even, odd = (eo[comp, k, par] + parts[par] for par in range(2))
                    result[comp, :, k * W:(k + 1) * W] = even + odd
                    result[comp, :, H + k * W:H + (k + 1) * W] = even - odd
                else:
                    for par in range(2):
                        eo[comp, k, par] = parts[par]

        repeat(2, component)

    back_y(0, False)
    back_y(1, True)

    to_mate().wait_send()
    for o in range(1, Z):
        pair_to(o).wait_send()
    for o in range(1, Y):
        row_to(o).wait_send()

    def sent(h):
        for x_to, c_to in x_peers():
            a_copy(h, x_to, c_to).wait_send()
            b_copy(h, x_to, c_to).wait_send()
        for z_to in z_peers():
            z_copy(h, z_to).wait_send()
            p_copy(h, z_to).wait_send()
        for o in range(1, Y):
            y_copy(h, o).wait_send()

    repeat(CHUNKS, sent)


def call(sizes, residual, counts, high, low):
    Y, Z, X, N = sizes
    m, H, W, B = N // X, N // 2, N // 4, N // Z
    vmem, dma = pltpu.VMEM, pltpu.SemaphoreType.DMA
    tile = vmem((8, LANES), F32)
    return pl.pallas_call(
        functools.partial(kernel, sizes),
        out_shape=jax.ShapeDtypeStruct((2, m, N), F32),
        in_specs=[pl.BlockSpec(memory_space=pltpu.SMEM)] + [pl.BlockSpec(memory_space=pltpu.HBM)] * 3,
        out_specs=pl.BlockSpec(memory_space=pltpu.VMEM),
        scratch_shapes=[
            vmem((2, m, N), F32),
            vmem((2, 2, H, W), BF16), vmem((2, 2, H, W), BF16),
            vmem((2, 2, 2, W, W), BF16), vmem((2, 2, 2, W, W), BF16),
            vmem((2, 2, m, H), BF16), vmem((2, 2, m, H), BF16),
            vmem((CHUNKS, X, 2, m // 2, LANES), F32),
            vmem((CHUNKS, 2, X, m // 2, LANES), F32),
            vmem((2, H, 2 * LANES), BF16),
            vmem((CHUNKS, N, LANES), F32),
            vmem((CHUNKS, Z, B // 2, LANES), F32),
            vmem((CHUNKS, N, LANES), F32), vmem((CHUNKS, N, LANES), F32),
            vmem((CHUNKS, Z, B // 2, LANES), F32),
            vmem((CHUNKS, B // 2, LANES), F32), vmem((CHUNKS, Y, B // 2, LANES), F32),
            vmem((CHUNKS, Z, B // 2, LANES), F32), vmem((CHUNKS, Z, B // 2, LANES), F32),
            vmem((N, 2 * LANES), BF16),
            vmem((CHUNKS, X, 2, m // 2, LANES), F32), vmem((CHUNKS, X, 2, m // 2, LANES), F32),
            vmem((2, 2, m, W), BF16), vmem((2, 2, m, W), BF16),
            vmem((2, 2, 2, m, W), F32),
            tile, tile, tile, vmem((Z, 8, LANES), F32), tile, vmem((Y, 8, LANES), F32),
            dma((3,)),
            dma((CHUNKS, X, 2)), dma((CHUNKS, X, 2)),
            dma((CHUNKS, Z)), dma((CHUNKS, Z)),
            dma((CHUNKS, Y)), dma((CHUNKS, Y)),
            dma((CHUNKS, Z)), dma((CHUNKS, Z)),
            dma((CHUNKS, X, 2)), dma((CHUNKS, X, 2)),
            dma, dma, dma((Z,)), dma((Z,)), dma((Y,)), dma((Y,)),
            pltpu.SemaphoreType.REGULAR, pltpu.SemaphoreType.REGULAR,
        ],
        compiler_params=pltpu.CompilerParams(
            collective_id=0, has_side_effects=True, vmem_limit_bytes=44 * 1024 * 1024
        ),
        name="wave",
    )(counts, *(pltpu.with_memory_space_constraint(a, pltpu.HBM) for a in (residual, high, low)))


def built(split, length):
    sizes = tuple(split.shape[a] for a in ("y", "z", "x")) + (length,)
    high, low = cas_tables(length)

    def on_device(residual, counts):
        return call(sizes, residual[0], counts, jnp.asarray(high), jnp.asarray(low))[None]

    times = ("y", "z", "c")
    return jax.shard_map(
        on_device,
        mesh=split,
        in_specs=(P(times, None, "x", None), P(times)),
        out_specs=P(times, None, "x", None),
        check_vma=False,
    )


def solution(mesh):
    points, spaces = mesh.shape["tm"], mesh.shape["space"]
    split = Mesh(mesh.devices.reshape(4, points // 8, 2, spaces), ("y", "z", "c", "x"))
    return built(split, 1024)
```

```python
import functools
import math

import jax
import jax.numpy as jnp
import numpy as np
from jax import lax
from jax.experimental import pallas as pl
from jax.experimental.pallas import tpu as pltpu
from jax.sharding import Mesh
from jax.sharding import PartitionSpec as P

phase_rate = 0.004
F32 = jnp.float32
BF16 = jnp.bfloat16
MESH = pl.DeviceIdType.MESH
LANES = 128
FOLD = 32
CHUNKS = 4

SIN_TERMS = [(-1) ** i * math.pi ** (2 * i + 1) / math.factorial(2 * i + 1) for i in range(7)]
COS_TERMS = [(-1) ** i * math.pi ** (2 * i) / math.factorial(2 * i) for i in range(7)]


def cas_tables(length):
    half, quarter = length // 2, length // 4
    place = np.arange(length)
    wave = 2 * (place % half) + place // half
    phases = (np.arange(half)[:, None] * wave[None, :] % length) * (2.0 * math.pi / length)
    table = np.cos(phases) + np.sin(phases)
    table = table.reshape(half, 2, 2, quarter).transpose(1, 2, 0, 3)
    high = table.astype(BF16)
    low = (table - high.astype(np.float64)).astype(BF16)
    return high, low


def halves(x):
    high = x.astype(BF16)
    return high, (x - high.astype(F32)).astype(BF16)


def dot3(a_high, a_low, b_high, b_low):
    dot = functools.partial(jnp.dot, preferred_element_type=F32)
    return dot(a_high, b_high) + (dot(a_low, b_high) + dot(a_high, b_low))


def product(high, low, packed):
    dot = functools.partial(jnp.dot, preferred_element_type=F32)
    both = dot(high, packed)
    return both[:, :LANES] + (both[:, LANES:] + dot(low, packed[:, :LANES]))


def signed(wave, length):
    return jnp.where(wave < length // 2, wave, wave - length).astype(F32)


def kernel(
    sizes,
    count_ref, source, table_high, table_low, result,
    r, th, tl, xh, xl, sdh, sdl, sa, rb, mix, own, fs, cosines, sines, zb, tt, ty, ps, pb,
    q, xs, yb, lh, ll, eo, c_own, c_mate, c_pair, c_z, c_row, c_y,
    load_sem, a_send, a_recv, z_send, z_recv, y_send, y_recv, p_send, p_recv, b_send, b_recv,
    cm_send, cm_recv, cz_send, cz_recv, cy_send, cy_recv, ready, go,
):
    Y, Z, X, N = sizes
    m, H, W, B, XH = N // X, N // 2, N // 4, N // Z, X // 2
    nb, m2, B2 = W // B, m // 2, B // 2
    yi, zi, ci, xi = (lax.axis_index(a) for a in ("y", "z", "c", "x"))
    mate = 1 - ci
    lane = lax.broadcasted_iota(jnp.int32, (1, LANES), 1)
    first_half = lane < 2 * FOLD
    w_lanes = lax.rem(lane, 2 * FOLD) < FOLD

    def turn(x, lanes):
        return pltpu.roll(x, lanes, axis=1)

    def swap(x):
        return jnp.where(w_lanes, turn(x, LANES - FOLD), turn(x, FOLD))

    def cross(a, b):
        return jnp.where(first_half, a, turn(b, 2 * FOLD)), jnp.where(first_half, turn(a, 2 * FOLD), b)

    def weave(a, b):
        return jnp.where(w_lanes, a, turn(b, FOLD)), jnp.where(w_lanes, turn(a, LANES - FOLD), b)

    def remote(src, dst, send, recv, **where):
        return pltpu.make_async_remote_copy(
            src_ref=src, dst_ref=dst, send_sem=send, recv_sem=recv, device_id=where, device_id_type=MESH
        )

    def x_peers():
        return [(lax.rem(xi + o, X), lax.rem(ci + d, 2)) for o in range(X) for d in range(2) if o or d]

    def z_peers():
        order = sorted(range(1, Z), key=lambda o: -min(o, Z - o))
        return [lax.rem(zi + o, Z) for o in order]

    def chunks(total, rows, body):
        def step(i, carry):
            body(pl.multiple_of(i * rows, rows))
            return carry
        lax.fori_loop(0, total // rows, step, 0)

    def repeat(count, body):
        def step(i, carry):
            body(i)
            return carry
        lax.fori_loop(0, count, step, 0)

    loads = [
        pltpu.make_async_copy(source, r, load_sem.at[0]),
        pltpu.make_async_copy(table_high, th, load_sem.at[1]),
        pltpu.make_async_copy(table_low, tl, load_sem.at[2]),
    ]
    for load in loads:
        load.start()

    barrier = pltpu.get_barrier_semaphore()
    lead = jnp.logical_and(xi == 0, ci == 1)
    for x_to, c_to in x_peers():
        @pl.when(jnp.logical_not(jnp.logical_and(x_to == 0, c_to == 1)))
        def _():
            pl.semaphore_signal(barrier, inc=1, device_id={"x": x_to, "c": c_to}, device_id_type=MESH)

    def group_is_here():
        @pl.when(jnp.logical_not(lead))
        def _():
            pl.semaphore_wait(barrier, 2 * X - 1)

        @pl.when(jnp.logical_and(xi == 0, ci == 0))
        def _():
            pl.semaphore_signal(ready, inc=1, device_id={"c": mate}, device_id_type=MESH)

        @pl.when(lead)
        def _():
            pl.semaphore_wait(ready, 1)
            for z_to in z_peers():
                pl.semaphore_signal(barrier, inc=1, device_id={"z": z_to}, device_id_type=MESH)
            for o in range(1, Y):
                pl.semaphore_signal(barrier, inc=1, device_id={"y": lax.rem(yi + o, Y)}, device_id_type=MESH)

    def all_are_here():
        @pl.when(lead)
        def _():
            pl.semaphore_wait(barrier, Z - 1 + Y - 1)
            for x_to, c_to in x_peers():
                pl.semaphore_signal(go, inc=1, device_id={"x": x_to, "c": c_to}, device_id_type=MESH)

        @pl.when(jnp.logical_not(lead))
        def _():
            pl.semaphore_wait(go, 1)

    def to_mate():
        return remote(c_own, c_mate, cm_send, cm_recv, c=mate)

    def pair_to(o):
        return remote(c_pair, c_z.at[o], cz_send.at[o], cz_recv.at[o], z=lax.rem(zi + o, Z))

    def row_to(o):
        return remote(c_row, c_y.at[o], cy_send.at[o], cy_recv.at[o], y=lax.rem(yi + o, Y))

    def fold_rows(par):
        sign = jnp.where(par == 0, 1.0, -1.0)
        for comp in range(2):
            def split_rows(at, comp=comp):
                rows = pl.ds(at, 32)
                sdh[par, comp, rows, :], sdl[par, comp, rows, :] = halves(r[comp, rows, :H] + sign * r[comp, rows, H:])
            chunks(m, 32, split_rows)

    loads[0].wait()
    fold_rows(1 - xi // XH)
    loads[1].wait()
    loads[2].wait()

    def a_copy(h, x_to, c_to):
        return remote(sa.at[h, x_to, c_to], rb.at[h, ci, xi], a_send.at[h, x_to, c_to], a_recv.at[h, xi, ci], x=x_to, c=c_to)

    def a_arrival(h, x_from, c_from):
        return remote(sa.at[h, x_from, c_from], rb.at[h, c_from, x_from], a_send.at[h, x_from, c_from],
                      a_recv.at[h, x_from, c_from], x=x_from, c=c_from)

    def along_y(i):
        pair, par = i // 2, lax.rem(xi // XH + 1 + i, 2)
        w_part = dot3(sdh[par, 0], sdl[par, 0], th[par, pair], tl[par, pair])
        v_part = dot3(sdh[par, 1], sdl[par, 1], th[par, pair], tl[par, pair])
        for j in range(2):
            lanes = slice(j * LANES, (j + 1) * LANES)
            w_tiles = cross(w_part[:m2, lanes], w_part[m2:, lanes])
            v_tiles = cross(v_part[:m2, lanes], v_part[m2:, lanes])
            for k in range(XH):
                sa[2 * pair + j, par * XH + k, 0], sa[2 * pair + j, par * XH + k, 1] = weave(w_tiles[k], v_tiles[k])

    def send_along_y(h, q):
        par = lax.rem(xi // XH + 1 + q, 2)
        for k in range(XH):
            x_to = par * XH + k

            @pl.when(x_to != xi)
            def _():
                a_copy(h, x_to, mate).start()
                a_copy(h, x_to, ci).start()

            @pl.when(x_to == xi)
            def _():
                a_copy(h, x_to, mate).start()
                rb[h, ci, xi] = sa[h, x_to, ci]

    c_own[...] = jnp.full(c_own.shape, count_ref[0].astype(F32), F32)
    along_y(0)
    group_is_here()
    to_mate().start()
    send_along_y(0, 0)
    fold_rows(xi // XH)
    along_y(1)
    for h, side in ((0, 1), (1, 0), (1, 1)):
        send_along_y(h, side)
    all_are_here()
    to_mate().wait_recv()
    c_pair[...] = c_own[...] + c_mate[...]
    for o in range(1, Z):
        pair_to(o).start()
    for side in range(2):
        along_y(2 + side)
    for h in (2, 3):
        for side in range(2):
            send_along_y(h, side)

    base = jnp.zeros_like(c_own)
    row = c_pair[...]
    for o in range(1, Z):
        pair_to(o).wait_recv()
        row = row + c_z[o]
        base = base + jnp.where(zi >= o, c_z[o], 0.0)
    c_row[...] = row
    for o in range(1, Y):
        row_to(o).start()

    for par in range(2):
        for h in range(2):
            for k in range(2):
                xh[par, h, k] = th[par, h, k * W:(k + 1) * W, :].astype(F32).T.astype(BF16)
                xl[par, h, k] = tl[par, h, k * W:(k + 1) * W, :].astype(F32).T.astype(BF16)

    for o in range(1, Y):
        row_to(o).wait_recv()
        base = base + jnp.where(yi >= o, c_y[o], 0.0)
    first_count = jnp.where(ci == 0, c_own[...], c_mate[...])
    rates = jnp.where(first_half, (base + first_count)[:1], (base + c_pair[...])[:1]) * (phase_rate / math.pi)
    terms = [jnp.where(w_lanes, s, c) for s, c in zip(SIN_TERMS, COS_TERMS)]
    column = lax.rem(lane, FOLD)

    def angles(h):
        col = h * LANES + lax.rem(xi, XH) * 2 * FOLD + ci * FOLD + column
        wave_y = signed(2 * col + xi // XH, N)

        def rows_of(at):
            place = at + lax.broadcasted_iota(jnp.int32, (64, LANES), 0)
            wave_x = signed(2 * lax.rem(place, H) + place // H, N)
            turns = jnp.sqrt(wave_x * wave_x + wave_y * wave_y) * rates
            nearest = jnp.floor(turns + 0.5)
            f = turns - nearest
            g = f * f
            value = terms[-1]
            for term in terms[-2::-1]:
                value = value * g + term
            value = jnp.where(w_lanes, value * f, value)
            half = nearest * 0.5
            value = jnp.where(half == jnp.floor(half), value, -value)
            other = swap(value)
            cosines[h, pl.ds(at, 64), :] = jnp.where(w_lanes, other, value)
            sines[h, pl.ds(at, 64), :] = jnp.where(w_lanes, -value, other)
        chunks(N, 64, rows_of)

    def z_copy(h, z_to):
        return remote(fs.at[h, z_to], zb.at[h, zi], z_send.at[h, z_to], z_recv.at[h, zi], z=z_to)

    def z_arrival(h, z_from):
        return remote(zb.at[h, z_from], zb.at[h, z_from], z_send.at[h, z_from], z_recv.at[h, z_from], z=z_from)

    def along_x(h):
        for x_from, c_from in x_peers():
            a_arrival(h, x_from, c_from).wait_recv()
        for k in range(XH):
            def split_rows(at, k=k):
                def place(par, half, x):
                    rows = pl.ds(pl.multiple_of(k * m + half * m2 + at, 64), 64)
                    mix[par, rows, :LANES], mix[par, rows, LANES:] = halves(x)
                near = [rb[h, t, k, pl.ds(at, 64), :] for t in range(2)]
                far = [rb[h, t, k + XH, pl.ds(at, 64), :] for t in range(2)]
                for half, x in enumerate(cross(near[0] + far[0], near[1] + far[1])):
                    place(0, half, x)
                for half, x in enumerate(cross(near[0] - far[0], near[1] - far[1])):
                    place(1, half, x)
            chunks(m2, 64, split_rows)

        def quarter(i):
            g = lax.rem(zi // nb + jnp.where(i < 2, 2 - i, 9 - 3 * i), 4)
            par, half = g // 2, lax.rem(g, 2)
            high = jnp.concatenate([xh[par, half, 0], xh[par, half, 1]], axis=1)
            low = jnp.concatenate([xl[par, half, 0], xl[par, half, 1]], axis=1)
            found = product(high, low, mix[par])
            rows = pl.ds(pl.multiple_of(g * W, W), W)
            framed = cosines[h, rows] * found + sines[h, rows] * swap(found)
            framed = framed + jnp.where(first_half, 0.0, turn(framed, 2 * FOLD))
            own[h, rows] = framed
            for k in range(nb):
                z_to = g * nb + k
                a, b = framed[k * B:k * B + B2], framed[k * B + B2:(k + 1) * B]
                fs[h, z_to] = jnp.where(first_half, turn(a, 2 * FOLD), b)
            for k in range(nb):
                z_to = g * nb + k

                @pl.when(z_to != zi)
                def _():
                    z_copy(h, z_to).start()

                @pl.when(z_to == zi)
                def _():
                    zb[h, zi] = fs[h, zi]

        repeat(4, quarter)

    def y_copy(h, o):
        return remote(tt.at[h], ty.at[h, o], y_send.at[h, o], y_recv.at[h, o], y=lax.rem(yi + o, Y))

    def p_copy(h, z_to):
        return remote(ps.at[h, z_to], pb.at[h, zi], p_send.at[h, z_to], p_recv.at[h, zi], z=z_to)

    def p_arrival(h, z_from):
        return remote(ps.at[h, z_from], pb.at[h, z_from], p_send.at[h, z_from], p_recv.at[h, z_from], z=z_from)

    def totals(h):
        for z_from in z_peers():
            z_arrival(h, z_from).wait_recv()
        total = zb[h, 0]
        for k in range(1, Z):
            total = total + zb[h, k]
        tt[h] = total
        for o in range(1, Y):
            y_copy(h, o).start()

    def prefix(h):
        for o in range(1, Y):
            y_copy(h, o).wait_recv()
        running = jnp.zeros((B2, LANES), F32)
        for o in range(1, Y):
            running = running + jnp.where(yi >= o, ty[h, o], 0.0)
        for k in range(Z):
            ps[h, k] = running
            running = running + zb[h, k]
        for z_to in z_peers():
            p_copy(h, z_to).start()
        pb[h, zi] = ps[h, zi]

    def forward(i):
        angles(i)
        along_x(i)

    repeat(3, forward)
    totals(0)
    forward(3)

    prefix(0)

    def middle(i):
        totals(i + 1)
        prefix(i + 1)

    repeat(3, middle)

    def b_copy(h, x_to, t):
        return remote(xs.at[h, x_to, t], yb.at[h, xi, ci], b_send.at[h, x_to, t], b_recv.at[h, xi, ci], x=x_to, c=t)

    def b_arrival(h, x_from, c_from):
        return remote(xs.at[h, x_from, c_from], yb.at[h, x_from, c_from], b_send.at[h, x_from, c_from],
                      b_recv.at[h, x_from, c_from], x=x_from, c=c_from)

    def back_x(h):
        def band(k):
            before = pb[h, k]
            for half, x in enumerate(cross(before, before)):
                rows = pl.ds(pl.multiple_of(k * B + half * B2, B2), B2)
                state = x + own[h, rows, :]
                state = cosines[h, rows, :] * state - sines[h, rows, :] * swap(state)
                q[rows, :LANES], q[rows, LANES:] = halves(state * (1.0 / (N * N)))

        band(zi)
        for z_from in z_peers():
            p_arrival(h, z_from).wait_recv()
            band(z_from)

        def block(i):
            k = lax.rem(xi + i, XH)
            rows = pl.ds(pl.multiple_of(k * m, m), m)
            parts = []
            for par in range(2):
                high = jnp.concatenate([th[par, 0, rows], th[par, 1, rows]], axis=1)
                low = jnp.concatenate([tl[par, 0, rows], tl[par, 1, rows]], axis=1)
                parts.append(product(high, low, q[par * H:(par + 1) * H]))
            for j, out in enumerate((parts[0] + parts[1], parts[0] - parts[1])):
                xs[h, k + j * XH, 0], xs[h, k + j * XH, 1] = cross(out[:m2], out[m2:])
            for j in range(2):
                x_to = k + j * XH

                @pl.when(x_to != xi)
                def _():
                    b_copy(h, x_to, mate).start()
                    b_copy(h, x_to, ci).start()

                @pl.when(x_to == xi)
                def _():
                    b_copy(h, x_to, mate).start()
                    yb[h, xi, ci] = xs[h, x_to, ci]

        repeat(XH, block)

    repeat(CHUNKS, back_x)

    def back_y(pair, last):
        for j in range(2):
            for x_from, c_from in x_peers():
                b_arrival(2 * pair + j, x_from, c_from).wait_recv()
            for par in range(2):
                def split_rows(at, par=par, j=j):
                    tiles = [weave(yb[2 * pair + j, par * XH + k, 0, pl.ds(at, 64), :],
                                   yb[2 * pair + j, par * XH + k, 1, pl.ds(at, 64), :]) for k in range(XH)]
                    lanes = slice(j * LANES, (j + 1) * LANES)
                    for comp in range(2):
                        for half, x in enumerate(cross(tiles[0][comp], tiles[1][comp])):
                            rows = pl.ds(pl.multiple_of(half * m2 + at, 64), 64)
                            lh[par, comp, rows, lanes], ll[par, comp, rows, lanes] = halves(x)
                chunks(m2, 64, split_rows)

        def component(comp):
            for k in range(2):
                parts = [dot3(lh[par, comp], ll[par, comp], xh[par, pair, k], xl[par, pair, k]) for par in range(2)]
                if last:
                    even, odd = (eo[comp, k, par] + parts[par] for par in range(2))
                    result[comp, :, k * W:(k + 1) * W] = even + odd
                    result[comp, :, H + k * W:H + (k + 1) * W] = even - odd
                else:
                    for par in range(2):
                        eo[comp, k, par] = parts[par]

        repeat(2, component)

    back_y(0, False)
    back_y(1, True)

    to_mate().wait_send()
    for o in range(1, Z):
        pair_to(o).wait_send()
    for o in range(1, Y):
        row_to(o).wait_send()

    def sent(h):
        for x_to, c_to in x_peers():
            a_copy(h, x_to, c_to).wait_send()
            b_copy(h, x_to, c_to).wait_send()
        for z_to in z_peers():
            z_copy(h, z_to).wait_send()
            p_copy(h, z_to).wait_send()
        for o in range(1, Y):
            y_copy(h, o).wait_send()

    repeat(CHUNKS, sent)


def call(sizes, residual, counts, high, low):
    Y, Z, X, N = sizes
    m, H, W, B = N // X, N // 2, N // 4, N // Z
    vmem, dma = pltpu.VMEM, pltpu.SemaphoreType.DMA
    tile = vmem((8, LANES), F32)
    return pl.pallas_call(
        functools.partial(kernel, sizes),
        out_shape=jax.ShapeDtypeStruct((2, m, N), F32),
        in_specs=[pl.BlockSpec(memory_space=pltpu.SMEM)] + [pl.BlockSpec(memory_space=pltpu.HBM)] * 3,
        out_specs=pl.BlockSpec(memory_space=pltpu.VMEM),
        scratch_shapes=[
            vmem((2, m, N), F32),
            vmem((2, 2, H, W), BF16), vmem((2, 2, H, W), BF16),
            vmem((2, 2, 2, W, W), BF16), vmem((2, 2, 2, W, W), BF16),
            vmem((2, 2, m, H), BF16), vmem((2, 2, m, H), BF16),
            vmem((CHUNKS, X, 2, m // 2, LANES), F32),
            vmem((CHUNKS, 2, X, m // 2, LANES), F32),
            vmem((2, H, 2 * LANES), BF16),
            vmem((CHUNKS, N, LANES), F32),
            vmem((CHUNKS, Z, B // 2, LANES), F32),
            vmem((CHUNKS, N, LANES), F32), vmem((CHUNKS, N, LANES), F32),
            vmem((CHUNKS, Z, B // 2, LANES), F32),
            vmem((CHUNKS, B // 2, LANES), F32), vmem((CHUNKS, Y, B // 2, LANES), F32),
            vmem((CHUNKS, Z, B // 2, LANES), F32), vmem((CHUNKS, Z, B // 2, LANES), F32),
            vmem((N, 2 * LANES), BF16),
            vmem((CHUNKS, X, 2, m // 2, LANES), F32), vmem((CHUNKS, X, 2, m // 2, LANES), F32),
            vmem((2, 2, m, W), BF16), vmem((2, 2, m, W), BF16),
            vmem((2, 2, 2, m, W), F32),
            tile, tile, tile, vmem((Z, 8, LANES), F32), tile, vmem((Y, 8, LANES), F32),
            dma((3,)),
            dma((CHUNKS, X, 2)), dma((CHUNKS, X, 2)),
            dma((CHUNKS, Z)), dma((CHUNKS, Z)),
            dma((CHUNKS, Y)), dma((CHUNKS, Y)),
            dma((CHUNKS, Z)), dma((CHUNKS, Z)),
            dma((CHUNKS, X, 2)), dma((CHUNKS, X, 2)),
            dma, dma, dma((Z,)), dma((Z,)), dma((Y,)), dma((Y,)),
            pltpu.SemaphoreType.REGULAR, pltpu.SemaphoreType.REGULAR,
        ],
        compiler_params=pltpu.CompilerParams(
            collective_id=0, has_side_effects=True, vmem_limit_bytes=44 * 1024 * 1024
        ),
        name="wave",
    )(counts, *(pltpu.with_memory_space_constraint(a, pltpu.HBM) for a in (residual, high, low)))


def built(split, length):
    sizes = tuple(split.shape[a] for a in ("y", "z", "x")) + (length,)
    high, low = cas_tables(length)

    def on_device(residual, counts):
        return call(sizes, residual[0], counts, jnp.asarray(high), jnp.asarray(low))[None]

    times = ("y", "z", "c")
    return jax.shard_map(
        on_device,
        mesh=split,
        in_specs=(P(times, None, "x", None), P(times)),
        out_specs=P(times, None, "x", None),
        check_vma=False,
    )


def solution(mesh):
    points, spaces = mesh.shape["tm"], mesh.shape["space"]
    split = Mesh(mesh.devices.reshape(4, points // 8, 2, spaces), ("y", "z", "c", "x"))
    return built(split, 1024)
```

```python
import functools
import math

import jax
import jax.numpy as jnp
import numpy as np
from jax import lax
from jax.experimental import pallas as pl
from jax.experimental.pallas import tpu as pltpu
from jax.sharding import Mesh
from jax.sharding import PartitionSpec as P

phase_rate = 0.004
F32 = jnp.float32
BF16 = jnp.bfloat16
MESH = pl.DeviceIdType.MESH
LANES = 128
FOLD = 32
CHUNKS = 4

SIN_TERMS = [(-1) ** i * math.pi ** (2 * i + 1) / math.factorial(2 * i + 1) for i in range(7)]
COS_TERMS = [(-1) ** i * math.pi ** (2 * i) / math.factorial(2 * i) for i in range(7)]


def cas_tables(length):
    half, quarter = length // 2, length // 4
    place = np.arange(length)
    wave = 2 * (place % half) + place // half
    phases = (np.arange(half)[:, None] * wave[None, :] % length) * (2.0 * math.pi / length)
    table = np.cos(phases) + np.sin(phases)
    table = table.reshape(half, 2, 2, quarter).transpose(1, 2, 0, 3)
    high = table.astype(BF16)
    low = (table - high.astype(np.float64)).astype(BF16)
    return high, low


def halves(x):
    high = x.astype(BF16)
    return high, (x - high.astype(F32)).astype(BF16)


def dot3(a_high, a_low, b_high, b_low):
    dot = functools.partial(jnp.dot, preferred_element_type=F32)
    return dot(a_high, b_high) + (dot(a_low, b_high) + dot(a_high, b_low))


def product(high, low, packed):
    dot = functools.partial(jnp.dot, preferred_element_type=F32)
    both = dot(high, packed)
    return both[:, :LANES] + (both[:, LANES:] + dot(low, packed[:, :LANES]))


def signed(wave, length):
    return jnp.where(wave < length // 2, wave, wave - length).astype(F32)


def kernel(
    sizes,
    count_ref, source, table_high, table_low, result,
    r, th, tl, xh, xl, sdh, sdl, sa, rb, mix, own, fs, cosines, sines, zb, tt, ty, ps, pb,
    q, xs, yb, lh, ll, eo, c_own, c_mate, c_pair, c_z, c_row, c_y,
    load_sem, a_send, a_recv, z_send, z_recv, y_send, y_recv, p_send, p_recv, b_send, b_recv,
    cm_send, cm_recv, cz_send, cz_recv, cy_send, cy_recv, ready, go,
):
    Y, Z, X, N = sizes
    m, H, W, B, XH = N // X, N // 2, N // 4, N // Z, X // 2
    nb, m2, B2 = W // B, m // 2, B // 2
    yi, zi, ci, xi = (lax.axis_index(a) for a in ("y", "z", "c", "x"))
    mate = 1 - ci
    lane = lax.broadcasted_iota(jnp.int32, (1, LANES), 1)
    first_half = lane < 2 * FOLD
    w_lanes = lax.rem(lane, 2 * FOLD) < FOLD

    def turn(x, lanes):
        return pltpu.roll(x, lanes, axis=1)

    def swap(x):
        return jnp.where(w_lanes, turn(x, LANES - FOLD), turn(x, FOLD))

    def cross(a, b):
        return jnp.where(first_half, a, turn(b, 2 * FOLD)), jnp.where(first_half, turn(a, 2 * FOLD), b)

    def weave(a, b):
        return jnp.where(w_lanes, a, turn(b, FOLD)), jnp.where(w_lanes, turn(a, LANES - FOLD), b)

    def remote(src, dst, send, recv, **where):
        return pltpu.make_async_remote_copy(
            src_ref=src, dst_ref=dst, send_sem=send, recv_sem=recv, device_id=where, device_id_type=MESH
        )

    def x_peers():
        return [(lax.rem(xi + o, X), lax.rem(ci + d, 2)) for o in range(X) for d in range(2) if o or d]

    def z_peers():
        order = sorted(range(1, Z), key=lambda o: -min(o, Z - o))
        return [lax.rem(zi + o, Z) for o in order]

    def chunks(total, rows, body):
        def step(i, carry):
            body(pl.multiple_of(i * rows, rows))
            return carry
        lax.fori_loop(0, total // rows, step, 0)

    def repeat(count, body):
        def step(i, carry):
            body(i)
            return carry
        lax.fori_loop(0, count, step, 0)

    loads = [
        pltpu.make_async_copy(source, r, load_sem.at[0]),
        pltpu.make_async_copy(table_high, th, load_sem.at[1]),
        pltpu.make_async_copy(table_low, tl, load_sem.at[2]),
    ]
    for load in loads:
        load.start()

    barrier = pltpu.get_barrier_semaphore()
    lead = jnp.logical_and(xi == 0, ci == 1)
    for x_to, c_to in x_peers():
        @pl.when(jnp.logical_not(jnp.logical_and(x_to == 0, c_to == 1)))
        def _():
            pl.semaphore_signal(barrier, inc=1, device_id={"x": x_to, "c": c_to}, device_id_type=MESH)

    def group_is_here():
        @pl.when(jnp.logical_not(lead))
        def _():
            pl.semaphore_wait(barrier, 2 * X - 1)

        @pl.when(jnp.logical_and(xi == 0, ci == 0))
        def _():
            pl.semaphore_signal(ready, inc=1, device_id={"c": mate}, device_id_type=MESH)

        @pl.when(lead)
        def _():
            pl.semaphore_wait(ready, 1)
            for z_to in z_peers():
                pl.semaphore_signal(barrier, inc=1, device_id={"z": z_to}, device_id_type=MESH)
            for o in range(1, Y):
                pl.semaphore_signal(barrier, inc=1, device_id={"y": lax.rem(yi + o, Y)}, device_id_type=MESH)

    def all_are_here():
        @pl.when(lead)
        def _():
            pl.semaphore_wait(barrier, Z - 1 + Y - 1)
            for x_to, c_to in x_peers():
                pl.semaphore_signal(go, inc=1, device_id={"x": x_to, "c": c_to}, device_id_type=MESH)

        @pl.when(jnp.logical_not(lead))
        def _():
            pl.semaphore_wait(go, 1)

    def to_mate():
        return remote(c_own, c_mate, cm_send, cm_recv, c=mate)

    def pair_to(o):
        return remote(c_pair, c_z.at[o], cz_send.at[o], cz_recv.at[o], z=lax.rem(zi + o, Z))

    def row_to(o):
        return remote(c_row, c_y.at[o], cy_send.at[o], cy_recv.at[o], y=lax.rem(yi + o, Y))

    def fold_rows(par):
        sign = jnp.where(par == 0, 1.0, -1.0)
        for comp in range(2):
            def split_rows(at, comp=comp):
                rows = pl.ds(at, 32)
                sdh[par, comp, rows, :], sdl[par, comp, rows, :] = halves(r[comp, rows, :H] + sign * r[comp, rows, H:])
            chunks(m, 32, split_rows)

    loads[0].wait()
    fold_rows(1 - xi // XH)
    loads[1].wait()
    loads[2].wait()

    def a_copy(h, x_to, c_to):
        return remote(sa.at[h, x_to, c_to], rb.at[h, ci, xi], a_send.at[h, x_to, c_to], a_recv.at[h, xi, ci], x=x_to, c=c_to)

    def a_arrival(h, x_from, c_from):
        return remote(sa.at[h, x_from, c_from], rb.at[h, c_from, x_from], a_send.at[h, x_from, c_from],
                      a_recv.at[h, x_from, c_from], x=x_from, c=c_from)

    def along_y(i):
        pair, par = i // 2, lax.rem(xi // XH + 1 + i, 2)
        w_part = dot3(sdh[par, 0], sdl[par, 0], th[par, pair], tl[par, pair])
        v_part = dot3(sdh[par, 1], sdl[par, 1], th[par, pair], tl[par, pair])
        for j in range(2):
            lanes = slice(j * LANES, (j + 1) * LANES)
            w_tiles = cross(w_part[:m2, lanes], w_part[m2:, lanes])
            v_tiles = cross(v_part[:m2, lanes], v_part[m2:, lanes])
            for k in range(XH):
                sa[2 * pair + j, par * XH + k, 0], sa[2 * pair + j, par * XH + k, 1] = weave(w_tiles[k], v_tiles[k])

    def send_along_y(h, q):
        par = lax.rem(xi // XH + 1 + q, 2)
        for k in range(XH):
            x_to = par * XH + k

            @pl.when(x_to != xi)
            def _():
                a_copy(h, x_to, mate).start()
                a_copy(h, x_to, ci).start()

            @pl.when(x_to == xi)
            def _():
                a_copy(h, x_to, mate).start()
                rb[h, ci, xi] = sa[h, x_to, ci]

    c_own[...] = jnp.full(c_own.shape, count_ref[0].astype(F32), F32)
    along_y(0)
    group_is_here()
    to_mate().start()
    send_along_y(0, 0)
    fold_rows(xi // XH)
    along_y(1)
    for h, side in ((0, 1), (1, 0), (1, 1)):
        send_along_y(h, side)
    all_are_here()
    to_mate().wait_recv()
    c_pair[...] = c_own[...] + c_mate[...]
    for o in range(1, Z):
        pair_to(o).start()
    for side in range(2):
        along_y(2 + side)
    for h in (2, 3):
        for side in range(2):
            send_along_y(h, side)

    base = jnp.zeros_like(c_own)
    row = c_pair[...]
    for o in range(1, Z):
        pair_to(o).wait_recv()
        row = row + c_z[o]
        base = base + jnp.where(zi >= o, c_z[o], 0.0)
    c_row[...] = row
    for o in range(1, Y):
        row_to(o).start()

    for par in range(2):
        for h in range(2):
            for k in range(2):
                xh[par, h, k] = th[par, h, k * W:(k + 1) * W, :].astype(F32).T.astype(BF16)
                xl[par, h, k] = tl[par, h, k * W:(k + 1) * W, :].astype(F32).T.astype(BF16)

    for o in range(1, Y):
        row_to(o).wait_recv()
        base = base + jnp.where(yi >= o, c_y[o], 0.0)
    first_count = jnp.where(ci == 0, c_own[...], c_mate[...])
    rates = jnp.where(first_half, (base + first_count)[:1], (base + c_pair[...])[:1]) * (phase_rate / math.pi)
    terms = [jnp.where(w_lanes, s, c) for s, c in zip(SIN_TERMS, COS_TERMS)]
    column = lax.rem(lane, FOLD)
    rows_apart = (2 * lax.broadcasted_iota(jnp.int32, (64, LANES), 0)).astype(F32)

    def angles(h):
        col = h * LANES + lax.rem(xi, XH) * 2 * FOLD + ci * FOLD + column
        wave_y = signed(2 * col + xi // XH, N)
        wave_y_squared = wave_y * wave_y

        def rows_of(at):
            wave_x = rows_apart + signed(2 * lax.rem(at, H) + at // H, N)
            turns = jnp.sqrt(wave_x * wave_x + wave_y_squared) * rates
            nearest = jnp.floor(turns + 0.5)
            f = turns - nearest
            g = f * f
            value = terms[-1]
            for term in terms[-2::-1]:
                value = value * g + term
            value = jnp.where(w_lanes, value * f, value)
            half = nearest * 0.5
            value = jnp.where(half == jnp.floor(half), value, -value)
            other = swap(value)
            cosines[h, pl.ds(at, 64), :] = jnp.where(w_lanes, other, value)
            sines[h, pl.ds(at, 64), :] = jnp.where(w_lanes, -value, other)
        chunks(N, 64, rows_of)

    def z_copy(h, z_to):
        return remote(fs.at[h, z_to], zb.at[h, zi], z_send.at[h, z_to], z_recv.at[h, zi], z=z_to)

    def z_arrival(h, z_from):
        return remote(zb.at[h, z_from], zb.at[h, z_from], z_send.at[h, z_from], z_recv.at[h, z_from], z=z_from)

    def along_x(h):
        for x_from, c_from in x_peers():
            a_arrival(h, x_from, c_from).wait_recv()
        for k in range(XH):
            def split_rows(at, k=k):
                def place(par, half, x):
                    rows = pl.ds(pl.multiple_of(k * m + half * m2 + at, 64), 64)
                    mix[par, rows, :LANES], mix[par, rows, LANES:] = halves(x)
                near = [rb[h, t, k, pl.ds(at, 64), :] for t in range(2)]
                far = [rb[h, t, k + XH, pl.ds(at, 64), :] for t in range(2)]
                for half, x in enumerate(cross(near[0] + far[0], near[1] + far[1])):
                    place(0, half, x)
                for half, x in enumerate(cross(near[0] - far[0], near[1] - far[1])):
                    place(1, half, x)
            chunks(m2, 64, split_rows)

        def quarter(i):
            g = lax.rem(zi // nb + jnp.where(i < 2, 2 - i, 9 - 3 * i), 4)
            par, half = g // 2, lax.rem(g, 2)
            high = jnp.concatenate([xh[par, half, 0], xh[par, half, 1]], axis=1)
            low = jnp.concatenate([xl[par, half, 0], xl[par, half, 1]], axis=1)
            found = product(high, low, mix[par])
            rows = pl.ds(pl.multiple_of(g * W, W), W)
            framed = cosines[h, rows] * found + sines[h, rows] * swap(found)
            framed = framed + jnp.where(first_half, 0.0, turn(framed, 2 * FOLD))
            own[h, rows] = framed
            for k in range(nb):
                z_to = g * nb + k
                a, b = framed[k * B:k * B + B2], framed[k * B + B2:(k + 1) * B]
                fs[h, z_to] = jnp.where(first_half, turn(a, 2 * FOLD), b)
            for k in range(nb):
                z_to = g * nb + k

                @pl.when(z_to != zi)
                def _():
                    z_copy(h, z_to).start()

                @pl.when(z_to == zi)
                def _():
                    zb[h, zi] = fs[h, zi]

        repeat(4, quarter)

    def y_copy(h, o):
        return remote(tt.at[h], ty.at[h, o], y_send.at[h, o], y_recv.at[h, o], y=lax.rem(yi + o, Y))

    def p_copy(h, z_to):
        return remote(ps.at[h, z_to], pb.at[h, zi], p_send.at[h, z_to], p_recv.at[h, zi], z=z_to)

    def p_arrival(h, z_from):
        return remote(ps.at[h, z_from], pb.at[h, z_from], p_send.at[h, z_from], p_recv.at[h, z_from], z=z_from)

    def totals(h):
        for z_from in z_peers():
            z_arrival(h, z_from).wait_recv()
        total = zb[h, 0]
        for k in range(1, Z):
            total = total + zb[h, k]
        tt[h] = total
        for o in range(1, Y):
            y_copy(h, o).start()

    def prefix(h):
        for o in range(1, Y):
            y_copy(h, o).wait_recv()
        running = jnp.zeros((B2, LANES), F32)
        for o in range(1, Y):
            running = running + jnp.where(yi >= o, ty[h, o], 0.0)
        for k in range(Z):
            ps[h, k] = running
            running = running + zb[h, k]
        for z_to in z_peers():
            p_copy(h, z_to).start()
        pb[h, zi] = ps[h, zi]

    def forward(i):
        angles(i)
        along_x(i)

    repeat(3, forward)
    totals(0)
    forward(3)

    prefix(0)

    def middle(i):
        totals(i + 1)
        prefix(i + 1)

    repeat(3, middle)

    def b_copy(h, x_to, t):
        return remote(xs.at[h, x_to, t], yb.at[h, xi, ci], b_send.at[h, x_to, t], b_recv.at[h, xi, ci], x=x_to, c=t)

    def b_arrival(h, x_from, c_from):
        return remote(xs.at[h, x_from, c_from], yb.at[h, x_from, c_from], b_send.at[h, x_from, c_from],
                      b_recv.at[h, x_from, c_from], x=x_from, c=c_from)

    def back_x(h):
        def band(k):
            before = pb[h, k]
            for half, x in enumerate(cross(before, before)):
                rows = pl.ds(pl.multiple_of(k * B + half * B2, B2), B2)
                state = x + own[h, rows, :]
                state = cosines[h, rows, :] * state - sines[h, rows, :] * swap(state)
                q[rows, :LANES], q[rows, LANES:] = halves(state * (1.0 / (N * N)))

        band(zi)
        for z_from in z_peers():
            p_arrival(h, z_from).wait_recv()
            band(z_from)

        def block(i):
            k = lax.rem(xi + i, XH)
            rows = pl.ds(pl.multiple_of(k * m, m), m)
            parts = []
            for par in range(2):
                high = jnp.concatenate([th[par, 0, rows], th[par, 1, rows]], axis=1)
                low = jnp.concatenate([tl[par, 0, rows], tl[par, 1, rows]], axis=1)
                parts.append(product(high, low, q[par * H:(par + 1) * H]))
            for j, out in enumerate((parts[0] + parts[1], parts[0] - parts[1])):
                xs[h, k + j * XH, 0], xs[h, k + j * XH, 1] = cross(out[:m2], out[m2:])
            for j in range(2):
                x_to = k + j * XH

                @pl.when(x_to != xi)
                def _():
                    b_copy(h, x_to, mate).start()
                    b_copy(h, x_to, ci).start()

                @pl.when(x_to == xi)
                def _():
                    b_copy(h, x_to, mate).start()
                    yb[h, xi, ci] = xs[h, x_to, ci]

        repeat(XH, block)

    repeat(CHUNKS, back_x)

    def back_y(pair, last):
        for j in range(2):
            for x_from, c_from in x_peers():
                b_arrival(2 * pair + j, x_from, c_from).wait_recv()
            for par in range(2):
                def split_rows(at, par=par, j=j):
                    tiles = [weave(yb[2 * pair + j, par * XH + k, 0, pl.ds(at, 64), :],
                                   yb[2 * pair + j, par * XH + k, 1, pl.ds(at, 64), :]) for k in range(XH)]
                    lanes = slice(j * LANES, (j + 1) * LANES)
                    for comp in range(2):
                        for half, x in enumerate(cross(tiles[0][comp], tiles[1][comp])):
                            rows = pl.ds(pl.multiple_of(half * m2 + at, 64), 64)
                            lh[par, comp, rows, lanes], ll[par, comp, rows, lanes] = halves(x)
                chunks(m2, 64, split_rows)

        def component(comp):
            for k in range(2):
                parts = [dot3(lh[par, comp], ll[par, comp], xh[par, pair, k], xl[par, pair, k]) for par in range(2)]
                if last:
                    even, odd = (eo[comp, k, par] + parts[par] for par in range(2))
                    result[comp, :, k * W:(k + 1) * W] = even + odd
                    result[comp, :, H + k * W:H + (k + 1) * W] = even - odd
                else:
                    for par in range(2):
                        eo[comp, k, par] = parts[par]

        repeat(2, component)

    back_y(0, False)
    back_y(1, True)

    to_mate().wait_send()
    for o in range(1, Z):
        pair_to(o).wait_send()
    for o in range(1, Y):
        row_to(o).wait_send()

    def sent(h):
        for x_to, c_to in x_peers():
            a_copy(h, x_to, c_to).wait_send()
            b_copy(h, x_to, c_to).wait_send()
        for z_to in z_peers():
            z_copy(h, z_to).wait_send()
            p_copy(h, z_to).wait_send()
        for o in range(1, Y):
            y_copy(h, o).wait_send()

    repeat(CHUNKS, sent)


def call(sizes, residual, counts, high, low):
    Y, Z, X, N = sizes
    m, H, W, B = N // X, N // 2, N // 4, N // Z
    vmem, dma = pltpu.VMEM, pltpu.SemaphoreType.DMA
    tile = vmem((8, LANES), F32)
    return pl.pallas_call(
        functools.partial(kernel, sizes),
        out_shape=jax.ShapeDtypeStruct((2, m, N), F32),
        in_specs=[pl.BlockSpec(memory_space=pltpu.SMEM)] + [pl.BlockSpec(memory_space=pltpu.HBM)] * 3,
        out_specs=pl.BlockSpec(memory_space=pltpu.VMEM),
        scratch_shapes=[
            vmem((2, m, N), F32),
            vmem((2, 2, H, W), BF16), vmem((2, 2, H, W), BF16),
            vmem((2, 2, 2, W, W), BF16), vmem((2, 2, 2, W, W), BF16),
            vmem((2, 2, m, H), BF16), vmem((2, 2, m, H), BF16),
            vmem((CHUNKS, X, 2, m // 2, LANES), F32),
            vmem((CHUNKS, 2, X, m // 2, LANES), F32),
            vmem((2, H, 2 * LANES), BF16),
            vmem((CHUNKS, N, LANES), F32),
            vmem((CHUNKS, Z, B // 2, LANES), F32),
            vmem((CHUNKS, N, LANES), F32), vmem((CHUNKS, N, LANES), F32),
            vmem((CHUNKS, Z, B // 2, LANES), F32),
            vmem((CHUNKS, B // 2, LANES), F32), vmem((CHUNKS, Y, B // 2, LANES), F32),
            vmem((CHUNKS, Z, B // 2, LANES), F32), vmem((CHUNKS, Z, B // 2, LANES), F32),
            vmem((N, 2 * LANES), BF16),
            vmem((CHUNKS, X, 2, m // 2, LANES), F32), vmem((CHUNKS, X, 2, m // 2, LANES), F32),
            vmem((2, 2, m, W), BF16), vmem((2, 2, m, W), BF16),
            vmem((2, 2, 2, m, W), F32),
            tile, tile, tile, vmem((Z, 8, LANES), F32), tile, vmem((Y, 8, LANES), F32),
            dma((3,)),
            dma((CHUNKS, X, 2)), dma((CHUNKS, X, 2)),
            dma((CHUNKS, Z)), dma((CHUNKS, Z)),
            dma((CHUNKS, Y)), dma((CHUNKS, Y)),
            dma((CHUNKS, Z)), dma((CHUNKS, Z)),
            dma((CHUNKS, X, 2)), dma((CHUNKS, X, 2)),
            dma, dma, dma((Z,)), dma((Z,)), dma((Y,)), dma((Y,)),
            pltpu.SemaphoreType.REGULAR, pltpu.SemaphoreType.REGULAR,
        ],
        compiler_params=pltpu.CompilerParams(
            collective_id=0, has_side_effects=True, vmem_limit_bytes=44 * 1024 * 1024
        ),
        name="wave",
    )(counts, *(pltpu.with_memory_space_constraint(a, pltpu.HBM) for a in (residual, high, low)))


def built(split, length):
    sizes = tuple(split.shape[a] for a in ("y", "z", "x")) + (length,)
    high, low = cas_tables(length)

    def on_device(residual, counts):
        return call(sizes, residual[0], counts, jnp.asarray(high), jnp.asarray(low))[None]

    times = ("y", "z", "c")
    return jax.shard_map(
        on_device,
        mesh=split,
        in_specs=(P(times, None, "x", None), P(times)),
        out_specs=P(times, None, "x", None),
        check_vma=False,
    )


def solution(mesh):
    points, spaces = mesh.shape["tm"], mesh.shape["space"]
    split = Mesh(mesh.devices.reshape(4, points // 8, 2, spaces), ("y", "z", "c", "x"))
    return built(split, 1024)
```

```python
import functools
import math

import jax
import jax.numpy as jnp
import numpy as np
from jax import lax
from jax.experimental import pallas as pl
from jax.experimental.pallas import tpu as pltpu
from jax.sharding import Mesh
from jax.sharding import PartitionSpec as P

phase_rate = 0.004
F32 = jnp.float32
BF16 = jnp.bfloat16
MESH = pl.DeviceIdType.MESH
LANES = 128
FOLD = 32
CHUNKS = 4

SIN_TERMS = [(-1) ** i * math.pi ** (2 * i + 1) / math.factorial(2 * i + 1) for i in range(7)]
COS_TERMS = [(-1) ** i * math.pi ** (2 * i) / math.factorial(2 * i) for i in range(7)]


def cas_tables(length):
    half, quarter = length // 2, length // 4
    place = np.arange(length)
    wave = 2 * (place % half) + place // half
    phases = (np.arange(half)[:, None] * wave[None, :] % length) * (2.0 * math.pi / length)
    table = np.cos(phases) + np.sin(phases)
    table = table.reshape(half, 2, 2, quarter).transpose(1, 2, 0, 3)
    high = table.astype(BF16)
    low = (table - high.astype(np.float64)).astype(BF16)
    return high, low


def halves(x):
    high = x.astype(BF16)
    return high, (x - high.astype(F32)).astype(BF16)


def dot3(a_high, a_low, b_high, b_low):
    dot = functools.partial(jnp.dot, preferred_element_type=F32)
    return dot(a_high, b_high) + (dot(a_low, b_high) + dot(a_high, b_low))


def product(high, low, packed):
    dot = functools.partial(jnp.dot, preferred_element_type=F32)
    both = dot(high, packed)
    return both[:, :LANES] + (both[:, LANES:] + dot(low, packed[:, :LANES]))


def signed(wave, length):
    return jnp.where(wave < length // 2, wave, wave - length).astype(F32)


def kernel(
    sizes,
    count_ref, source, table_high, table_low, result,
    r, th, tl, xh, xl, sdh, sdl, sa, rb, mix, own, fs, cosines, sines, zb, tt, ty, ps, pb,
    q, xs, yb, lh, ll, eo, c_own, c_mate, c_pair, c_z, c_row, c_y,
    load_sem, a_send, a_recv, z_send, z_recv, y_send, y_recv, p_send, p_recv, b_send, b_recv,
    cm_send, cm_recv, cz_send, cz_recv, cy_send, cy_recv, ready, go,
):
    Y, Z, X, N = sizes
    m, H, W, B, XH = N // X, N // 2, N // 4, N // Z, X // 2
    nb, m2, B2 = W // B, m // 2, B // 2
    yi, zi, ci, xi = (lax.axis_index(a) for a in ("y", "z", "c", "x"))
    mate = 1 - ci
    lane = lax.broadcasted_iota(jnp.int32, (1, LANES), 1)
    first_half = lane < 2 * FOLD
    w_lanes = lax.rem(lane, 2 * FOLD) < FOLD

    def turn(x, lanes):
        return pltpu.roll(x, lanes, axis=1)

    def swap(x):
        return jnp.where(w_lanes, turn(x, LANES - FOLD), turn(x, FOLD))

    def cross(a, b):
        return jnp.where(first_half, a, turn(b, 2 * FOLD)), jnp.where(first_half, turn(a, 2 * FOLD), b)

    def weave(a, b):
        return jnp.where(w_lanes, a, turn(b, FOLD)), jnp.where(w_lanes, turn(a, LANES - FOLD), b)

    def remote(src, dst, send, recv, **where):
        return pltpu.make_async_remote_copy(
            src_ref=src, dst_ref=dst, send_sem=send, recv_sem=recv, device_id=where, device_id_type=MESH
        )

    def x_peers():
        return [(lax.rem(xi + o, X), lax.rem(ci + d, 2)) for o in range(X) for d in range(2) if o or d]

    def z_peers():
        order = sorted(range(1, Z), key=lambda o: -min(o, Z - o))
        return [lax.rem(zi + o, Z) for o in order]

    def chunks(total, rows, body):
        def step(i, carry):
            body(pl.multiple_of(i * rows, rows))
            return carry
        lax.fori_loop(0, total // rows, step, 0)

    def repeat(count, body):
        def step(i, carry):
            body(i)
            return carry
        lax.fori_loop(0, count, step, 0)

    loads = [
        pltpu.make_async_copy(source, r, load_sem.at[0]),
        pltpu.make_async_copy(table_high, th, load_sem.at[1]),
        pltpu.make_async_copy(table_low, tl, load_sem.at[2]),
    ]
    for load in loads:
        load.start()

    barrier = pltpu.get_barrier_semaphore()
    lead = jnp.logical_and(xi == 0, ci == 1)
    for x_to, c_to in x_peers():
        @pl.when(jnp.logical_not(jnp.logical_and(x_to == 0, c_to == 1)))
        def _():
            pl.semaphore_signal(barrier, inc=1, device_id={"x": x_to, "c": c_to}, device_id_type=MESH)

    def group_is_here():
        @pl.when(jnp.logical_not(lead))
        def _():
            pl.semaphore_wait(barrier, 2 * X - 1)

        @pl.when(jnp.logical_and(xi == 0, ci == 0))
        def _():
            pl.semaphore_signal(ready, inc=1, device_id={"c": mate}, device_id_type=MESH)

        @pl.when(lead)
        def _():
            pl.semaphore_wait(ready, 1)
            for z_to in z_peers():
                pl.semaphore_signal(barrier, inc=1, device_id={"z": z_to}, device_id_type=MESH)
            for o in range(1, Y):
                pl.semaphore_signal(barrier, inc=1, device_id={"y": lax.rem(yi + o, Y)}, device_id_type=MESH)

    def all_are_here():
        @pl.when(lead)
        def _():
            pl.semaphore_wait(barrier, Z - 1 + Y - 1)
            for x_to, c_to in x_peers():
                pl.semaphore_signal(go, inc=1, device_id={"x": x_to, "c": c_to}, device_id_type=MESH)

        @pl.when(jnp.logical_not(lead))
        def _():
            pl.semaphore_wait(go, 1)

    def to_mate():
        return remote(c_own, c_mate, cm_send, cm_recv, c=mate)

    def pair_to(o):
        return remote(c_pair, c_z.at[o], cz_send.at[o], cz_recv.at[o], z=lax.rem(zi + o, Z))

    def row_to(o):
        return remote(c_row, c_y.at[o], cy_send.at[o], cy_recv.at[o], y=lax.rem(yi + o, Y))

    def fold_rows(par):
        sign = jnp.where(par == 0, 1.0, -1.0)
        for comp in range(2):
            def split_rows(at, comp=comp):
                rows = pl.ds(at, 32)
                sdh[par, comp, rows, :], sdl[par, comp, rows, :] = halves(r[comp, rows, :H] + sign * r[comp, rows, H:])
            chunks(m, 32, split_rows)

    loads[0].wait()
    fold_rows(1 - xi // XH)
    loads[1].wait()
    loads[2].wait()

    def a_copy(h, x_to, c_to):
        return remote(sa.at[h, x_to, c_to], rb.at[h, ci, xi], a_send.at[h, x_to, c_to], a_recv.at[h, xi, ci], x=x_to, c=c_to)

    def a_arrival(h, x_from, c_from):
        return remote(sa.at[h, x_from, c_from], rb.at[h, c_from, x_from], a_send.at[h, x_from, c_from],
                      a_recv.at[h, x_from, c_from], x=x_from, c=c_from)

    def along_y(i):
        pair, par = i // 2, lax.rem(xi // XH + 1 + i, 2)
        w_part = dot3(sdh[par, 0], sdl[par, 0], th[par, pair], tl[par, pair])
        v_part = dot3(sdh[par, 1], sdl[par, 1], th[par, pair], tl[par, pair])
        for j in range(2):
            lanes = slice(j * LANES, (j + 1) * LANES)
            w_tiles = cross(w_part[:m2, lanes], w_part[m2:, lanes])
            v_tiles = cross(v_part[:m2, lanes], v_part[m2:, lanes])
            for k in range(XH):
                sa[2 * pair + j, par * XH + k, 0], sa[2 * pair + j, par * XH + k, 1] = weave(w_tiles[k], v_tiles[k])

    def send_along_y(h, q):
        par = lax.rem(xi // XH + 1 + q, 2)
        for k in range(XH):
            x_to = par * XH + k

            @pl.when(x_to != xi)
            def _():
                a_copy(h, x_to, mate).start()
                a_copy(h, x_to, ci).start()

            @pl.when(x_to == xi)
            def _():
                a_copy(h, x_to, mate).start()
                rb[h, ci, xi] = sa[h, x_to, ci]

    c_own[...] = jnp.full(c_own.shape, count_ref[0].astype(F32), F32)
    along_y(0)
    group_is_here()
    to_mate().start()
    send_along_y(0, 0)
    fold_rows(xi // XH)
    along_y(1)
    for h, side in ((0, 1), (1, 0), (1, 1)):
        send_along_y(h, side)
    all_are_here()
    to_mate().wait_recv()
    c_pair[...] = c_own[...] + c_mate[...]
    for o in range(1, Z):
        pair_to(o).start()
    for side in range(2):
        along_y(2 + side)
    for h in (2, 3):
        for side in range(2):
            send_along_y(h, side)

    base = jnp.zeros_like(c_own)
    row = c_pair[...]
    for o in range(1, Z):
        pair_to(o).wait_recv()
        row = row + c_z[o]
        base = base + jnp.where(zi >= o, c_z[o], 0.0)
    c_row[...] = row
    for o in range(1, Y):
        row_to(o).start()

    for par in range(2):
        for h in range(2):
            for k in range(2):
                xh[par, h, k] = th[par, h, k * W:(k + 1) * W, :].astype(F32).T.astype(BF16)
                xl[par, h, k] = tl[par, h, k * W:(k + 1) * W, :].astype(F32).T.astype(BF16)

    for o in range(1, Y):
        row_to(o).wait_recv()
        base = base + jnp.where(yi >= o, c_y[o], 0.0)
    first_count = jnp.where(ci == 0, c_own[...], c_mate[...])
    rates = jnp.where(first_half, (base + first_count)[:1], (base + c_pair[...])[:1]) * (phase_rate / math.pi)
    terms = [jnp.where(w_lanes, s, c) for s, c in zip(SIN_TERMS, COS_TERMS)]
    column = lax.rem(lane, FOLD)
    rows_apart = (2 * lax.broadcasted_iota(jnp.int32, (64, LANES), 0)).astype(F32)

    def angles(h):
        col = h * LANES + lax.rem(xi, XH) * 2 * FOLD + ci * FOLD + column
        wave_y = signed(2 * col + xi // XH, N)
        wave_y_squared = wave_y * wave_y

        def rows_of(at):
            wave_x = rows_apart + signed(2 * lax.rem(at, H) + at // H, N)
            turns = jnp.sqrt(wave_x * wave_x + wave_y_squared) * rates
            nearest = jnp.floor(turns + 0.5)
            f = turns - nearest
            g = f * f
            value = terms[-1]
            for term in terms[-2::-1]:
                value = value * g + term
            value = jnp.where(w_lanes, value * f, value)
            half = nearest * 0.5
            value = jnp.where(half == jnp.floor(half), value, -value)
            other = swap(value)
            cosines[h, pl.ds(at, 64), :] = jnp.where(w_lanes, other, value)
            sines[h, pl.ds(at, 64), :] = jnp.where(w_lanes, -value, other)
        chunks(N, 64, rows_of)

    def z_copy(h, z_to):
        return remote(fs.at[h, z_to], zb.at[h, zi], z_send.at[h, z_to], z_recv.at[h, zi], z=z_to)

    def z_arrival(h, z_from):
        return remote(zb.at[h, z_from], zb.at[h, z_from], z_send.at[h, z_from], z_recv.at[h, z_from], z=z_from)

    def along_x(h):
        for x_from, c_from in x_peers():
            a_arrival(h, x_from, c_from).wait_recv()
        for k in range(XH):
            def split_rows(at, k=k):
                def place(par, half, x):
                    rows = pl.ds(pl.multiple_of(k * m + half * m2 + at, 64), 64)
                    mix[par, rows, :LANES], mix[par, rows, LANES:] = halves(x)
                near = [rb[h, t, k, pl.ds(at, 64), :] for t in range(2)]
                far = [rb[h, t, k + XH, pl.ds(at, 64), :] for t in range(2)]
                for half, x in enumerate(cross(near[0] + far[0], near[1] + far[1])):
                    place(0, half, x)
                for half, x in enumerate(cross(near[0] - far[0], near[1] - far[1])):
                    place(1, half, x)
            chunks(m2, 64, split_rows)

        def quarter(i):
            g = lax.rem(zi // nb + jnp.where(i < 2, 2 - i, 9 - 3 * i), 4)
            par, half = g // 2, lax.rem(g, 2)
            high = jnp.concatenate([xh[par, half, 0], xh[par, half, 1]], axis=1)
            low = jnp.concatenate([xl[par, half, 0], xl[par, half, 1]], axis=1)
            found = product(high, low, mix[par])
            rows = pl.ds(pl.multiple_of(g * W, W), W)
            framed = cosines[h, rows] * found + sines[h, rows] * swap(found)
            framed = framed + jnp.where(first_half, 0.0, turn(framed, 2 * FOLD))
            own[h, rows] = framed
            for k in range(nb):
                z_to = g * nb + k
                a, b = framed[k * B:k * B + B2], framed[k * B + B2:(k + 1) * B]
                fs[h, z_to] = jnp.where(first_half, turn(a, 2 * FOLD), b)
            for k in range(nb):
                z_to = g * nb + k

                @pl.when(z_to != zi)
                def _():
                    z_copy(h, z_to).start()

                @pl.when(z_to == zi)
                def _():
                    zb[h, zi] = fs[h, zi]

        repeat(4, quarter)

    def y_copy(h, o):
        return remote(tt.at[h], ty.at[h, o], y_send.at[h, o], y_recv.at[h, o], y=lax.rem(yi + o, Y))

    def p_copy(h, z_to):
        return remote(ps.at[h, z_to], pb.at[h, zi], p_send.at[h, z_to], p_recv.at[h, zi], z=z_to)

    def p_arrival(h, z_from):
        return remote(ps.at[h, z_from], pb.at[h, z_from], p_send.at[h, z_from], p_recv.at[h, z_from], z=z_from)

    def totals(h):
        for z_from in z_peers():
            z_arrival(h, z_from).wait_recv()
        total = zb[h, 0]
        for k in range(1, Z):
            total = total + zb[h, k]
        tt[h] = total
        for o in range(1, Y):
            y_copy(h, o).start()

    def prefix(h):
        for o in range(1, Y):
            y_copy(h, o).wait_recv()
        running = jnp.zeros((B2, LANES), F32)
        for o in range(1, Y):
            running = running + jnp.where(yi >= o, ty[h, o], 0.0)
        for k in range(Z):
            ps[h, k] = running
            running = running + zb[h, k]
        for z_to in z_peers():
            p_copy(h, z_to).start()
        pb[h, zi] = ps[h, zi]

    def forward(i):
        angles(i)
        along_x(i)

    repeat(3, forward)
    totals(0)
    forward(3)

    prefix(0)

    def middle(i):
        totals(i + 1)
        prefix(i + 1)

    repeat(3, middle)

    def b_copy(h, x_to, t):
        return remote(xs.at[h, x_to, t], yb.at[h, xi, ci], b_send.at[h, x_to, t], b_recv.at[h, xi, ci], x=x_to, c=t)

    def b_arrival(h, x_from, c_from):
        return remote(xs.at[h, x_from, c_from], yb.at[h, x_from, c_from], b_send.at[h, x_from, c_from],
                      b_recv.at[h, x_from, c_from], x=x_from, c=c_from)

    def back_x(h):
        def band(k):
            before = pb[h, k]
            for half, x in enumerate(cross(before, before)):
                rows = pl.ds(pl.multiple_of(k * B + half * B2, B2), B2)
                state = x + own[h, rows, :]
                state = cosines[h, rows, :] * state - sines[h, rows, :] * swap(state)
                q[rows, :LANES], q[rows, LANES:] = halves(state * (1.0 / (N * N)))

        band(zi)
        for z_from in z_peers():
            p_arrival(h, z_from).wait_recv()
            band(z_from)

        def block(i):
            k = lax.rem(xi + i, XH)
            rows = pl.ds(pl.multiple_of(k * m, m), m)
            parts = []
            for par in range(2):
                high = jnp.concatenate([th[par, 0, rows], th[par, 1, rows]], axis=1)
                low = jnp.concatenate([tl[par, 0, rows], tl[par, 1, rows]], axis=1)
                parts.append(product(high, low, q[par * H:(par + 1) * H]))
            for j, out in enumerate((parts[0] + parts[1], parts[0] - parts[1])):
                xs[h, k + j * XH, 0], xs[h, k + j * XH, 1] = cross(out[:m2], out[m2:])
            for j in range(2):
                x_to = k + j * XH

                @pl.when(x_to != xi)
                def _():
                    b_copy(h, x_to, mate).start()
                    b_copy(h, x_to, ci).start()

                @pl.when(x_to == xi)
                def _():
                    b_copy(h, x_to, mate).start()
                    yb[h, xi, ci] = xs[h, x_to, ci]

        repeat(XH, block)

    repeat(CHUNKS, back_x)

    def back_y(pair, last):
        for j in range(2):
            for x_from, c_from in x_peers():
                b_arrival(2 * pair + j, x_from, c_from).wait_recv()
            for par in range(2):
                def split_rows(at, par=par, j=j):
                    tiles = [weave(yb[2 * pair + j, par * XH + k, 0, pl.ds(at, 64), :],
                                   yb[2 * pair + j, par * XH + k, 1, pl.ds(at, 64), :]) for k in range(XH)]
                    lanes = slice(j * LANES, (j + 1) * LANES)
                    for comp in range(2):
                        for half, x in enumerate(cross(tiles[0][comp], tiles[1][comp])):
                            rows = pl.ds(pl.multiple_of(half * m2 + at, 64), 64)
                            lh[par, comp, rows, lanes], ll[par, comp, rows, lanes] = halves(x)
                chunks(m2, 64, split_rows)
            if last:
                def accumulate(comp, j=j):
                    waves = slice(j * LANES, (j + 1) * LANES)
                    for k in range(2):
                        parts = []
                        for par in range(2):
                            high, low = lh[par, comp, :, waves], ll[par, comp, :, waves]
                            table = xh[par, pair, k, waves, :]
                            both = jnp.dot(jnp.concatenate([high, low], axis=1), jnp.concatenate([table, table], axis=0),
                                           preferred_element_type=F32)
                            rest = jnp.dot(high, xl[par, pair, k, waves, :], preferred_element_type=F32)
                            parts.append(eo[comp, k, par] + (both + rest))
                        if j == 0:
                            eo[comp, k, 0], eo[comp, k, 1] = parts
                        else:
                            result[comp, :, k * W:(k + 1) * W] = parts[0] + parts[1]
                            result[comp, :, H + k * W:H + (k + 1) * W] = parts[0] - parts[1]
                repeat(2, accumulate)

        def component(comp):
            for k in range(2):
                for par in range(2):
                    eo[comp, k, par] = dot3(lh[par, comp], ll[par, comp], xh[par, pair, k], xl[par, pair, k])

        if not last:
            repeat(2, component)

    back_y(0, False)
    back_y(1, True)

    to_mate().wait_send()
    for o in range(1, Z):
        pair_to(o).wait_send()
    for o in range(1, Y):
        row_to(o).wait_send()

    def sent(h):
        for x_to, c_to in x_peers():
            a_copy(h, x_to, c_to).wait_send()
            b_copy(h, x_to, c_to).wait_send()
        for z_to in z_peers():
            z_copy(h, z_to).wait_send()
            p_copy(h, z_to).wait_send()
        for o in range(1, Y):
            y_copy(h, o).wait_send()

    repeat(CHUNKS, sent)


def call(sizes, residual, counts, high, low):
    Y, Z, X, N = sizes
    m, H, W, B = N // X, N // 2, N // 4, N // Z
    vmem, dma = pltpu.VMEM, pltpu.SemaphoreType.DMA
    tile = vmem((8, LANES), F32)
    return pl.pallas_call(
        functools.partial(kernel, sizes),
        out_shape=jax.ShapeDtypeStruct((2, m, N), F32),
        in_specs=[pl.BlockSpec(memory_space=pltpu.SMEM)] + [pl.BlockSpec(memory_space=pltpu.HBM)] * 3,
        out_specs=pl.BlockSpec(memory_space=pltpu.VMEM),
        scratch_shapes=[
            vmem((2, m, N), F32),
            vmem((2, 2, H, W), BF16), vmem((2, 2, H, W), BF16),
            vmem((2, 2, 2, W, W), BF16), vmem((2, 2, 2, W, W), BF16),
            vmem((2, 2, m, H), BF16), vmem((2, 2, m, H), BF16),
            vmem((CHUNKS, X, 2, m // 2, LANES), F32),
            vmem((CHUNKS, 2, X, m // 2, LANES), F32),
            vmem((2, H, 2 * LANES), BF16),
            vmem((CHUNKS, N, LANES), F32),
            vmem((CHUNKS, Z, B // 2, LANES), F32),
            vmem((CHUNKS, N, LANES), F32), vmem((CHUNKS, N, LANES), F32),
            vmem((CHUNKS, Z, B // 2, LANES), F32),
            vmem((CHUNKS, B // 2, LANES), F32), vmem((CHUNKS, Y, B // 2, LANES), F32),
            vmem((CHUNKS, Z, B // 2, LANES), F32), vmem((CHUNKS, Z, B // 2, LANES), F32),
            vmem((N, 2 * LANES), BF16),
            vmem((CHUNKS, X, 2, m // 2, LANES), F32), vmem((CHUNKS, X, 2, m // 2, LANES), F32),
            vmem((2, 2, m, W), BF16), vmem((2, 2, m, W), BF16),
            vmem((2, 2, 2, m, W), F32),
            tile, tile, tile, vmem((Z, 8, LANES), F32), tile, vmem((Y, 8, LANES), F32),
            dma((3,)),
            dma((CHUNKS, X, 2)), dma((CHUNKS, X, 2)),
            dma((CHUNKS, Z)), dma((CHUNKS, Z)),
            dma((CHUNKS, Y)), dma((CHUNKS, Y)),
            dma((CHUNKS, Z)), dma((CHUNKS, Z)),
            dma((CHUNKS, X, 2)), dma((CHUNKS, X, 2)),
            dma, dma, dma((Z,)), dma((Z,)), dma((Y,)), dma((Y,)),
            pltpu.SemaphoreType.REGULAR, pltpu.SemaphoreType.REGULAR,
        ],
        compiler_params=pltpu.CompilerParams(
            collective_id=0, has_side_effects=True, vmem_limit_bytes=44 * 1024 * 1024
        ),
        name="wave",
    )(counts, *(pltpu.with_memory_space_constraint(a, pltpu.HBM) for a in (residual, high, low)))


def built(split, length):
    sizes = tuple(split.shape[a] for a in ("y", "z", "x")) + (length,)
    high, low = cas_tables(length)

    def on_device(residual, counts):
        return call(sizes, residual[0], counts, jnp.asarray(high), jnp.asarray(low))[None]

    times = ("y", "z", "c")
    return jax.shard_map(
        on_device,
        mesh=split,
        in_specs=(P(times, None, "x", None), P(times)),
        out_specs=P(times, None, "x", None),
        check_vma=False,
    )


def solution(mesh):
    points, spaces = mesh.shape["tm"], mesh.shape["space"]
    split = Mesh(mesh.devices.reshape(4, points // 8, 2, spaces), ("y", "z", "c", "x"))
    return built(split, 1024)
```
